128 devices in a mesh: rows: 16 (over y, x), dict: 8 (over z, core).
Axes of the slice: x: 4, y: 4, z: 4, core: 2. Of those that a mesh axis runs over, the one named last changes fastest.
Arguments:
- lookup_keys_per_record: int32 [524288], P(('rows', 'dict')), may hold values from 0 to 65535, as said below
- filter_passed_flags: int32 [524288], P(('rows', 'dict')), may hold values from 0 to 1
- decoding_table: bfloat16 [65536, 128], P('dict'), may hold values from -6 to 6
Outputs:
- compacted: bfloat16 [524288, 128], P(('rows', 'dict'))
The draws below stay inside these ranges and needn't reach their ends.
Inputs may be any that keep to these rules, and one draw needn't show every extreme that they name: Codes of the rows of one device lie in one range of 8192 consecutive lookup_keys_per_record (k * 8192 to (k + 1) * 8192 - 1) at most 1024 times, and exactly 1024 times for some range, whose rows all survive.
All inputs are finite; a program needn't handle non-finite values.
Results may differ from the reference program's by a relative error of at most 0.001.
Values may be sent and summed in bfloat16 or wider, within the bound.
No kernel may reach another device: no remote copies, remote signals or barrier semaphores. Data moves between devices by JAX's collectives and lax.ppermute only.
A program may use at most 64 MiB of HBM per device.

```python
import jax
import jax.numpy as jnp

W = 128
VD = 8192
RD = 4096
CAP = 1024
VOCAB = 65536
ROWS_ALL = 524288


def joint_draw(key):
    blocks = ROWS_ALL // RD
    ranges = VOCAB // VD
    keys = jax.random.split(jax.random.fold_in(key, 11), 6)
    hot_range = jax.random.randint(keys[0], (blocks, 1), 0, ranges)
    row_orderings = jax.vmap(lambda k: jax.random.permutation(k, RD))(jax.random.split(keys[1], blocks))
    spread = (row_orderings - CAP) % (ranges - 1)
    others = (hot_range + 1 + spread) % ranges
    forced = row_orderings < CAP
    owner = jnp.where(forced, hot_range, others)
    first = jax.random.randint(keys[3], (blocks, RD), 0, VD)
    second = jax.random.randint(keys[4], (blocks, RD), 0, VD)
    inner = first * second // VD
    lookup_keys_per_record = (owner * VD + inner).reshape(ROWS_ALL).astype(jnp.int32)
    run_length = max(1, blocks // 8)
    run_count = (blocks + run_length - 1) // run_length
    run_levels = jax.random.randint(keys[2], (run_count,), 1, 20).astype(jnp.int32)
    run_of_block = (jnp.arange(blocks, dtype=jnp.int32) // run_length).astype(jnp.int32)
    levels = jnp.take(run_levels, run_of_block, axis=0)[:, None]
    drawn = jax.random.randint(keys[5], (blocks, RD), 0, 20)
    alive = forced | (drawn < levels)
    return (lookup_keys_per_record, alive.astype(jnp.int32).reshape(ROWS_ALL))


def draw_lookup_keys_per_record(key, part):
    return joint_draw(key)[0]


def draw_filter_passed_flags(key, part):
    return joint_draw(key)[1]


def block_levels(rng, dims, cuts, least, largest):
    loudness, own = 1.0, jax.random.fold_in(rng, 6)
    for dim, blocks in cuts:
        heights = jnp.exp(jax.random.uniform(jax.random.fold_in(own, dim), (blocks,), jnp.float32, least / len(cuts), largest / len(cuts)))
        loudness = loudness * jnp.repeat(heights, dims[dim] // blocks).reshape([-1 if axis == dim else 1 for axis in range(len(dims))])
    return loudness


def gaussian(key, shape, scale, reach, shards=(), kind=jnp.bfloat16):
    array = jax.random.normal(key, shape, jnp.float32) * scale
    if len(shards) > 0:
        array = block_levels(key, shape, shards, -0.22, 0.18) * array
    return jnp.clip(array, min=-reach, max=reach).astype(kind)


def setup_inputs(seed: int = 0) -> dict:
    splits = jax.random.split(jax.random.key(seed), 4)
    lookup_keys_per_record = draw_lookup_keys_per_record(jax.random.fold_in(splits[3], 71), 0)
    filter_passed_flags = draw_filter_passed_flags(jax.random.fold_in(splits[3], 71), 0)
    decoding_table = gaussian(splits[2], (VOCAB, W), 1.0, 6.0, ((0, 8),))
    return {"lookup_keys_per_record": lookup_keys_per_record, "filter_passed_flags": filter_passed_flags, "decoding_table": decoding_table}


def reference(lookup_keys_per_record, filter_passed_flags, decoding_table):
    keeper_flags = filter_passed_flags > 0
    overall_position = (jnp.cumsum(filter_passed_flags) - 1).astype(jnp.int32)
    decoded = jnp.take(decoding_table, lookup_keys_per_record, axis=0)
    target = jnp.where(keeper_flags, overall_position, jnp.int32(ROWS_ALL)).astype(jnp.int32)
    empty = jnp.zeros((ROWS_ALL, W), decoding_table.dtype)
    return empty.at[target].set(decoded, mode="drop")
```

```python
import functools

import jax
import jax.numpy as jnp
from jax import lax
from jax.experimental import pallas as pl
from jax.experimental.pallas import tpu as pltpu
from jax.sharding import PartitionSpec as P

ALL = ("rows", "dict")
LANES = 128
PRESENT = 1 << 30
DEVICES = 128
BLOCKS = 32


def iota(shape, dim):
    return lax.broadcasted_iota(jnp.int32, shape, dim)


def exact_dot(a, b):
    return jnp.dot(a.astype(jnp.bfloat16), b.astype(jnp.bfloat16), preferred_element_type=jnp.float32)


def local_compaction(keys_ref, flags_ref, out_ref):
    flags = flags_ref[...]
    rows = flags.shape[0]
    upper = jnp.where(iota((LANES, LANES), 0) <= iota((LANES, LANES), 1), 1.0, 0.0)
    below = jnp.where(iota((rows, rows), 1) < iota((rows, rows), 0), 1.0, 0.0)
    kept = flags.astype(jnp.float32)
    inclusive = exact_dot(kept, upper)
    row_sums = exact_dot(kept, jnp.ones((LANES, LANES), jnp.float32))
    position = (inclusive + exact_dot(below, row_sums)).astype(jnp.int32) - 1
    count = jnp.sum(row_sums, axis=0, keepdims=True).astype(jnp.int32)
    here = iota((rows, LANES), 0) * LANES + iota((rows, LANES), 1)
    lane = iota((rows, LANES), 1)
    item = jnp.where(flags > 0, PRESENT | ((here - position) << 16) | keys_ref[...], 0)
    for level in range((rows * LANES - 1).bit_length()):
        step = 1 << level
        moving = (item >> (16 + level)) & 1 == 1
        sent = jnp.where(moving, item, 0)
        if step < LANES:
            near = pltpu.roll(sent, LANES - step, 1)
            arrived = jnp.where(lane < LANES - step, near, pltpu.roll(near, rows - 1, 0))
        else:
            arrived = pltpu.roll(sent, rows - step // LANES, 0)
        item = jnp.where(moving, 0, item) | arrived
    codes = item & 0xFFFF
    counts = jnp.broadcast_to(count, (LANES - rows, LANES))
    out_ref[...] = jnp.concatenate([codes, counts], axis=0).T


def regroup(me_ref, counts_ref, got_ref, out_ref, low_ref, high_ref, rows_ref):
    me = me_ref[0]
    got = got_ref[...]
    shape = got.shape
    lane = iota(shape, 1)
    count = jnp.max(jnp.where(lane >= BLOCKS, got, 0), axis=1, keepdims=True)
    count = jnp.broadcast_to(count, shape)
    below = jnp.where(iota(shape, 1) < iota(shape, 0), 1.0, 0.0)
    offset = 64 * exact_dot(below, (count >> 6).astype(jnp.float32)) + exact_dot(below, (count & 63).astype(jnp.float32))
    start = offset.astype(jnp.int32) + me
    valid = (lane < BLOCKS) & (lane * LANES + me < count)
    item = jnp.where(valid, PRESENT | ((start & 127) << 16) | got, 0)
    turn = (start >> 7) & (BLOCKS - 1)
    for level in range(5):
        item = jnp.where((turn >> level) & 1 == 1, pltpu.roll(item, 1 << level, 1), item)
    odd = iota(shape, 0) & 1 == 1
    low = jnp.where(lane < BLOCKS, item, 0)
    high = jnp.where(lane < BLOCKS, pltpu.roll(item, LANES - BLOCKS, 1), 0)
    low_ref[...] = jnp.where(odd, pltpu.roll(low, BLOCKS, 1), low)
    high_ref[...] = jnp.where(odd, pltpu.roll(high, BLOCKS, 1), high)
    rows_ref[...] = jnp.zeros_like(rows_ref)

    def place(s, before):
        d = (before + me) >> 12
        rows_ref[pl.ds(d, 1), :] = rows_ref[pl.ds(d, 1), :] | low_ref[pl.ds(s, 1), :]
        rows_ref[pl.ds(d + 1, 1), :] = rows_ref[pl.ds(d + 1, 1), :] | high_ref[pl.ds(s, 1), :]
        return before + counts_ref[s]

    lax.fori_loop(0, DEVICES, place, jnp.int32(0), unroll=8)
    out_ref[...] = rows_ref[:DEVICES, :]


def placement(got_ref, out_ref, *, absent):
    item = got_ref[...].T[: 2 * BLOCKS]
    lane = iota(item.shape, 1)
    turn = (((item >> 16) & 127) - lane) & 127
    item = jnp.where(item > 0, (item & (PRESENT | 0xFFFF)) | (turn << 16), 0)
    for level in range(7):
        moving = (item >> (16 + level)) & 1 == 1
        item = jnp.where(moving, 0, item) | pltpu.roll(jnp.where(moving, item, 0), 1 << level, 1)
    item = item[:BLOCKS] | item[BLOCKS:]
    out_ref[...] = jnp.where(item > 0, item & 0xFFFF, absent)


def decode(codes_ref, table_ref, out_ref, wide_ref, part_ref, staged_ref, sems):
    entries = table_ref.shape[0]
    slots, chunk = part_ref.shape[:2]
    chunks = entries // chunk

    def fetch(c):
        return pltpu.make_async_copy(
            table_ref.at[pl.ds(c * chunk, chunk)], part_ref.at[c % slots], sems.at[c % slots]
        )

    for c in range(slots):
        fetch(c).start()
    wide_ref[pl.ds(entries, 8), :] = jnp.zeros((8, LANES), jnp.float32)
    for c in range(chunks):
        fetch(c).wait()

        def widen(i, _, c=c):
            at = pl.multiple_of(i * 128, 128)
            to = pl.multiple_of(c * chunk + i * 128, 128)
            wide_ref[pl.ds(to, 128), :] = part_ref[c % slots, pl.ds(at, 128), :].astype(jnp.float32)
            return 0

        lax.fori_loop(0, chunk // 128, widen, 0)
        if c + slots < chunks:
            fetch(c + slots).start()

    def block(b, _):
        base = pl.multiple_of(b * LANES, LANES)
        for j in range(LANES):
            staged_ref[pl.ds(j, 1), :] = wide_ref[pl.ds(codes_ref[b, j], 1), :]
        out_ref[pl.ds(base, LANES), :] = staged_ref[...].astype(out_ref.dtype)
        return 0

    lax.fori_loop(0, BLOCKS, block, 0)


def vmem():
    return pl.BlockSpec(memory_space=pltpu.VMEM)


def smem():
    return pl.BlockSpec(memory_space=pltpu.SMEM)


def exchange(x):
    return lax.all_to_all(x, ALL, 0, 0, tiled=True)


def on_device(lookup_keys_per_record, filter_passed_flags, decoding_table):
    me = lax.axis_index(ALL).astype(jnp.int32).reshape(1)
    square = jax.ShapeDtypeStruct((DEVICES, LANES), jnp.int32)
    whole = lax.all_gather(decoding_table, "dict", axis=0, tiled=True)
    sent = pl.pallas_call(local_compaction, out_shape=square, in_specs=[vmem(), vmem()], out_specs=vmem(), name="local_compaction")(
        lookup_keys_per_record.reshape(BLOCKS, LANES), filter_passed_flags.reshape(BLOCKS, LANES)
    )
    got = exchange(sent)
    sent = pl.pallas_call(
        regroup,
        out_shape=square,
        in_specs=[smem(), smem(), vmem()],
        out_specs=vmem(),
        scratch_shapes=[pltpu.VMEM((DEVICES, LANES), jnp.int32)] * 2 + [pltpu.VMEM((DEVICES + 8, LANES), jnp.int32)],
        name="regroup",
    )(me, got[:, BLOCKS], got)
    got = exchange(sent)
    entries = whole.shape[0]
    codes = pl.pallas_call(
        functools.partial(placement, absent=entries),
        out_shape=jax.ShapeDtypeStruct((BLOCKS, LANES), jnp.int32),
        in_specs=[vmem()],
        out_specs=vmem(),
        name="placement",
    )(got)
    return pl.pallas_call(
        decode,
        out_shape=jax.ShapeDtypeStruct((BLOCKS * LANES, LANES), jnp.bfloat16),
        in_specs=[smem(), pl.BlockSpec(memory_space=pl.ANY)],
        out_specs=vmem(),
        scratch_shapes=[
            pltpu.VMEM((entries + 8, LANES), jnp.float32),
            pltpu.VMEM((4, 4096, LANES), jnp.bfloat16),
            pltpu.VMEM((LANES, LANES), jnp.float32),
            pltpu.SemaphoreType.DMA((4,)),
        ],
        compiler_params=pltpu.CompilerParams(vmem_limit_bytes=48 << 20),
        name="decode",
    )(codes, whole)


def solution(mesh):
    placed = (P(ALL), P(ALL), P("dict", None))
    return jax.shard_map(
        on_device, mesh=mesh, in_specs=placed, out_specs=P(ALL, None), check_vma=False
    )
```

```python
import functools

import jax
import jax.numpy as jnp
from jax import lax
from jax.experimental import pallas as pl
from jax.experimental.pallas import tpu as pltpu
from jax.sharding import PartitionSpec as P

ALL = ("rows", "dict")
LANES = 128
PRESENT = 1 << 30
DEVICES = 128
BLOCKS = 32
SHARD = 8192
PART = 768
CHUNK = 3 * PART
RING = (-1, 1, 2)


def iota(shape, dim):
    return lax.broadcasted_iota(jnp.int32, shape, dim)


def exact_dot(a, b):
    return jnp.dot(a.astype(jnp.bfloat16), b.astype(jnp.bfloat16), preferred_element_type=jnp.float32)


def local_compaction(keys_ref, flags_ref, out_ref):
    flags = flags_ref[...]
    rows = flags.shape[0]
    upper = jnp.where(iota((LANES, LANES), 0) <= iota((LANES, LANES), 1), 1.0, 0.0)
    below = jnp.where(iota((rows, rows), 1) < iota((rows, rows), 0), 1.0, 0.0)
    kept = flags.astype(jnp.float32)
    inclusive = exact_dot(kept, upper)
    row_sums = exact_dot(kept, jnp.ones((LANES, LANES), jnp.float32))
    position = (inclusive + exact_dot(below, row_sums)).astype(jnp.int32) - 1
    count = jnp.sum(row_sums, axis=0, keepdims=True).astype(jnp.int32)
    here = iota((rows, LANES), 0) * LANES + iota((rows, LANES), 1)
    lane = iota((rows, LANES), 1)
    item = jnp.where(flags > 0, PRESENT | ((here - position) << 16) | keys_ref[...], 0)
    for level in range((rows * LANES - 1).bit_length()):
        step = 1 << level
        moving = (item >> (16 + level)) & 1 == 1
        sent = jnp.where(moving, item, 0)
        if step < LANES:
            near = pltpu.roll(sent, LANES - step, 1)
            arrived = jnp.where(lane < LANES - step, near, pltpu.roll(near, rows - 1, 0))
        else:
            arrived = pltpu.roll(sent, rows - step // LANES, 0)
        item = jnp.where(moving, 0, item) | arrived
    codes = item & 0xFFFF
    counts = jnp.broadcast_to(count, (LANES - rows, LANES))
    out_ref[...] = jnp.concatenate([codes, counts], axis=0).T


def regroup(me_ref, counts_ref, got_ref, out_ref, low_ref, high_ref, rows_ref):
    me = me_ref[0]
    got = got_ref[...]
    shape = got.shape
    lane = iota(shape, 1)
    count = jnp.max(jnp.where(lane >= BLOCKS, got, 0), axis=1, keepdims=True)
    count = jnp.broadcast_to(count, shape)
    below = jnp.where(iota(shape, 1) < iota(shape, 0), 1.0, 0.0)
    offset = 64 * exact_dot(below, (count >> 6).astype(jnp.float32)) + exact_dot(below, (count & 63).astype(jnp.float32))
    start = offset.astype(jnp.int32) + me
    valid = (lane < BLOCKS) & (lane * LANES + me < count)
    item = jnp.where(valid, PRESENT | ((start & 127) << 16) | got, 0)
    turn = (start >> 7) & (BLOCKS - 1)
    for level in range(5):
        item = jnp.where((turn >> level) & 1 == 1, pltpu.roll(item, 1 << level, 1), item)
    odd = iota(shape, 0) & 1 == 1
    low = jnp.where(lane < BLOCKS, item, 0)
    high = jnp.where(lane < BLOCKS, pltpu.roll(item, LANES - BLOCKS, 1), 0)
    low_ref[...] = jnp.where(odd, pltpu.roll(low, BLOCKS, 1), low)
    high_ref[...] = jnp.where(odd, pltpu.roll(high, BLOCKS, 1), high)
    rows_ref[...] = jnp.zeros_like(rows_ref)

    def place(s, before):
        d = (before + me) >> 12
        rows_ref[pl.ds(d, 1), :] = rows_ref[pl.ds(d, 1), :] | low_ref[pl.ds(s, 1), :]
        rows_ref[pl.ds(d + 1, 1), :] = rows_ref[pl.ds(d + 1, 1), :] | high_ref[pl.ds(s, 1), :]
        return before + counts_ref[s]

    lax.fori_loop(0, DEVICES, place, jnp.int32(0), unroll=8)
    out_ref[...] = rows_ref[:DEVICES, :]


def placement(got_ref, out_ref, *, absent):
    item = got_ref[...].T[: 2 * BLOCKS]
    lane = iota(item.shape, 1)
    turn = (((item >> 16) & 127) - lane) & 127
    item = jnp.where(item > 0, (item & (PRESENT | 0xFFFF)) | (turn << 16), 0)
    for level in range(7):
        moving = (item >> (16 + level)) & 1 == 1
        item = jnp.where(moving, 0, item) | pltpu.roll(jnp.where(moving, item, 0), 1 << level, 1)
    item = item[:BLOCKS] | item[BLOCKS:]
    out_ref[...] = jnp.where(item > 0, item & 0xFFFF, absent)


def table_parts(me, half):
    x, y, z, core = (me >> 3) & 3, me >> 5, (me >> 1) & 3, (me & 1) ^ half
    around = [(z + step) & 3 for step in RING]
    bases = [(other * 2 + core) * SHARD for other in around]
    parts = [[(SHARD, (z * 2 + core) * SHARD)]]
    parts += [[(PART, base + PART * x) for base in bases], [(PART, base + 4 * PART + PART * y) for base in bases]]
    parts += [[(SHARD - 8 * PART, base + 8 * PART)] for base in bases]
    parts += [[(PART, base + PART * ((x + step) & 3)) for base in bases] for step in RING]
    parts += [[(PART, base + 4 * PART + PART * ((y + step) & 3)) for base in bases] for step in RING]
    return parts


def decode(me_ref, codes_ref, *refs):
    pieces, (out_ref, wide_ref, part_ref, staged_ref, sems) = refs[:-5], refs[-5:]
    me = me_ref[0]
    parts = table_parts(me, 0) + table_parts(me, 1)
    slots = part_ref.shape[0]
    work = []
    for piece, places in zip(pieces, parts):
        rows = piece.shape[0]
        if len(places) == 1:
            for at in range(0, rows, CHUNK):
                work.append((piece, at, min(CHUNK, rows - at), [(min(CHUNK, rows - at), places[0][1] + at)]))
        else:
            work.append((piece, 0, rows, places))

    def fetch(i):
        piece, at, rows, _ = work[i]
        return pltpu.make_async_copy(
            piece.at[pl.ds(at, rows)], part_ref.at[i % slots, pl.ds(0, rows)], sems.at[i % slots]
        )

    for i in range(slots):
        fetch(i).start()
    entries = wide_ref.shape[0] - 8
    wide_ref[pl.ds(entries, 8), :] = jnp.zeros((8, LANES), jnp.float32)
    for i, (_, _, _, places) in enumerate(work):
        fetch(i).wait()
        done = 0
        for rows, base in places:

            def widen(step, _, done=done, base=base, i=i):
                at = pl.multiple_of(done + step * LANES, LANES)
                to = pl.multiple_of(base + step * LANES, LANES)
                wide_ref[pl.ds(to, LANES), :] = part_ref[i % slots, pl.ds(at, LANES), :].astype(jnp.float32)
                return 0

            lax.fori_loop(0, rows // LANES, widen, 0)
            done += rows
        if i + slots < len(work):
            fetch(i + slots).start()

    def block(b, _):
        base = pl.multiple_of(b * LANES, LANES)
        for j in range(LANES):
            staged_ref[pl.ds(j, 1), :] = wide_ref[pl.ds(codes_ref[b, j], 1), :]
        out_ref[pl.ds(base, LANES), :] = staged_ref[...].astype(out_ref.dtype)
        return 0

    lax.fori_loop(0, BLOCKS, block, 0)


def moved(x, by):
    pairs = []
    for me in range(DEVICES):
        place = ((me >> 3) & 3, me >> 5, (me >> 1) & 3, me & 1)
        to_x, to_y, to_z, to_core = by(*place)
        pairs.append((me, ((to_y & 3) * 4 + (to_x & 3)) * 8 + (to_z & 3) * 2 + to_core))
    return lax.ppermute(x, ALL, pairs)


def along_x(piece):
    return [moved(piece, lambda x, y, z, core, step=step: (x - step, y, z, core)) for step in RING]


def along_y(piece):
    return [moved(piece, lambda x, y, z, core, step=step: (x, y - step, z, core)) for step in RING]


def along_z(piece):
    return [moved(piece, lambda x, y, z, core, step=step: (x, y, z - step, core)) for step in RING]


def other_core(piece):
    return moved(piece, lambda x, y, z, core: (x, y, z, 1 - core))


def first_pieces(table):
    row = lax.axis_index("rows")
    x, y = row & 3, row >> 2
    quarters = [
        lax.dynamic_slice_in_dim(table, PART * x, PART, 0),
        lax.dynamic_slice_in_dim(table, 4 * PART + PART * y, PART, 0),
    ]
    return along_z(jnp.concatenate(quarters, axis=0)), along_z(table[8 * PART :])


def later_pieces(first):
    for_x = jnp.concatenate([piece[:PART] for piece in first], axis=0)
    for_y = jnp.concatenate([piece[PART:] for piece in first], axis=0)
    return for_x, for_y, along_x(for_x), along_y(for_y)


def vmem():
    return pl.BlockSpec(memory_space=pltpu.VMEM)


def smem():
    return pl.BlockSpec(memory_space=pltpu.SMEM)


def exchange(x):
    return lax.all_to_all(x, ALL, 0, 0, tiled=True)


def on_device(lookup_keys_per_record, filter_passed_flags, decoding_table):
    me = lax.axis_index(ALL).astype(jnp.int32).reshape(1)
    square = jax.ShapeDtypeStruct((DEVICES, LANES), jnp.int32)
    first, rest = first_pieces(decoding_table)
    other_table = other_core(decoding_table)
    sent = pl.pallas_call(local_compaction, out_shape=square, in_specs=[vmem(), vmem()], out_specs=vmem(), name="local_compaction")(
        lookup_keys_per_record.reshape(BLOCKS, LANES), filter_passed_flags.reshape(BLOCKS, LANES)
    )
    got, first = lax.optimization_barrier((exchange(sent), first))
    for_x, for_y, from_x, from_y = later_pieces(first)
    other_xy = [other_core(for_x), other_core(for_y)]
    sent = pl.pallas_call(
        regroup,
        out_shape=square,
        in_specs=[smem(), smem(), vmem()],
        out_specs=vmem(),
        scratch_shapes=[pltpu.VMEM((DEVICES, LANES), jnp.int32)] * 2 + [pltpu.VMEM((DEVICES + 8, LANES), jnp.int32)],
        name="regroup",
    )(me, got[:, BLOCKS], got)
    got, rest, from_x, from_y = lax.optimization_barrier((exchange(sent), rest, from_x, from_y))
    late = [*rest, *from_x, *from_y]
    pieces = [decoding_table, for_x, for_y, *late, other_table, *other_xy, *(other_core(piece) for piece in late)]
    entries = 8 * SHARD
    codes = pl.pallas_call(
        functools.partial(placement, absent=entries),
        out_shape=jax.ShapeDtypeStruct((BLOCKS, LANES), jnp.int32),
        in_specs=[vmem()],
        out_specs=vmem(),
        name="placement",
    )(got)
    return pl.pallas_call(
        decode,
        out_shape=jax.ShapeDtypeStruct((BLOCKS * LANES, LANES), jnp.bfloat16),
        in_specs=[smem(), smem()] + [pl.BlockSpec(memory_space=pl.ANY)] * len(pieces),
        out_specs=vmem(),
        scratch_shapes=[
            pltpu.VMEM((entries + 8, LANES), jnp.float32),
            pltpu.VMEM((4, CHUNK, LANES), jnp.bfloat16),
            pltpu.VMEM((LANES, LANES), jnp.float32),
            pltpu.SemaphoreType.DMA((4,)),
        ],
        compiler_params=pltpu.CompilerParams(vmem_limit_bytes=48 << 20),
        name="decode",
    )(me, codes, *pieces)


def solution(mesh):
    placed = (P(ALL), P(ALL), P("dict", None))
    return jax.shard_map(
        on_device, mesh=mesh, in_specs=placed, out_specs=P(ALL, None), check_vma=False
    )
```

```python
import functools

import jax
import jax.numpy as jnp
from jax import lax
from jax.experimental import pallas as pl
from jax.experimental.pallas import tpu as pltpu
from jax.sharding import PartitionSpec as P


ALL = ("rows", "dict")
LANES = 128
PRESENT = 1 << 30
DEVICES = 128
BLOCKS = 32
SHARD = 8192
PART = 768
CHUNK = 3 * PART
RING = (-1, 1, 2)


def iota(shape, dim):
    return lax.broadcasted_iota(jnp.int32, shape, dim)


def exact_dot(a, b):
    return jnp.dot(a.astype(jnp.bfloat16), b.astype(jnp.bfloat16), preferred_element_type=jnp.float32)


def local_compaction(keys_ref, flags_ref, out_ref):
    flags = flags_ref[...]
    rows = flags.shape[0]
    upper = jnp.where(iota((LANES, LANES), 0) <= iota((LANES, LANES), 1), 1.0, 0.0)
    below = jnp.where(iota((rows, rows), 1) < iota((rows, rows), 0), 1.0, 0.0)
    kept = flags.astype(jnp.float32)
    inclusive = exact_dot(kept, upper)
    row_sums = exact_dot(kept, jnp.ones((LANES, LANES), jnp.float32))
    position = (inclusive + exact_dot(below, row_sums)).astype(jnp.int32) - 1
    count = jnp.sum(row_sums, axis=0, keepdims=True).astype(jnp.int32)
    here = iota((rows, LANES), 0) * LANES + iota((rows, LANES), 1)
    lane = iota((rows, LANES), 1)
    item = jnp.where(flags > 0, PRESENT | ((here - position) << 16) | keys_ref[...], 0)
    for level in range((rows * LANES - 1).bit_length()):
        step = 1 << level
        moving = (item >> (16 + level)) & 1 == 1
        sent = jnp.where(moving, item, 0)
        if step < LANES:
            near = pltpu.roll(sent, LANES - step, 1)
            arrived = jnp.where(lane < LANES - step, near, pltpu.roll(near, rows - 1, 0))
        else:
            arrived = pltpu.roll(sent, rows - step // LANES, 0)
        item = jnp.where(moving, 0, item) | arrived
    codes = item & 0xFFFF
    counts = jnp.broadcast_to(count, (LANES - rows, LANES))
    out_ref[...] = jnp.concatenate([codes, counts], axis=0).T


def regroup(me_ref, counts_ref, got_ref, out_ref, low_ref, high_ref, rows_ref):
    me = me_ref[0]
    got = got_ref[...]
    shape = got.shape
    lane = iota(shape, 1)
    count = jnp.max(jnp.where(lane >= BLOCKS, got, 0), axis=1, keepdims=True)
    count = jnp.broadcast_to(count, shape)
    below = jnp.where(iota(shape, 1) < iota(shape, 0), 1.0, 0.0)
    offset = 64 * exact_dot(below, (count >> 6).astype(jnp.float32)) + exact_dot(below, (count & 63).astype(jnp.float32))
    start = offset.astype(jnp.int32) + me
    valid = (lane < BLOCKS) & (lane * LANES + me < count)
    item = jnp.where(valid, PRESENT | ((start & 127) << 16) | got, 0)
    turn = (start >> 7) & (BLOCKS - 1)
    for level in range(5):
        item = jnp.where((turn >> level) & 1 == 1, pltpu.roll(item, 1 << level, 1), item)
    odd = iota(shape, 0) & 1 == 1
    low = jnp.where(lane < BLOCKS, item, 0)
    high = jnp.where(lane < BLOCKS, pltpu.roll(item, LANES - BLOCKS, 1), 0)
    low_ref[...] = jnp.where(odd, pltpu.roll(low, BLOCKS, 1), low)
    high_ref[...] = jnp.where(odd, pltpu.roll(high, BLOCKS, 1), high)
    rows_ref[...] = jnp.zeros_like(rows_ref)

    def place(s, before):
        d = (before + me) >> 12
        rows_ref[pl.ds(d, 1), :] = rows_ref[pl.ds(d, 1), :] | low_ref[pl.ds(s, 1), :]
        rows_ref[pl.ds(d + 1, 1), :] = rows_ref[pl.ds(d + 1, 1), :] | high_ref[pl.ds(s, 1), :]
        return before + counts_ref[s]

    lax.fori_loop(0, DEVICES, place, jnp.int32(0), unroll=8)
    out_ref[...] = rows_ref[:DEVICES, :]


def placement(got_ref, out_ref, *, absent):
    item = got_ref[...].T[: 2 * BLOCKS]
    lane = iota(item.shape, 1)
    turn = (((item >> 16) & 127) - lane) & 127
    item = jnp.where(item > 0, (item & (PRESENT | 0xFFFF)) | (turn << 16), 0)
    for level in range(7):
        moving = (item >> (16 + level)) & 1 == 1
        item = jnp.where(moving, 0, item) | pltpu.roll(jnp.where(moving, item, 0), 1 << level, 1)
    item = item[:BLOCKS] | item[BLOCKS:]
    out_ref[...] = jnp.where(item > 0, item & 0xFFFF, absent)


def table_parts(me, half):
    x, y, z, core = (me >> 3) & 3, me >> 5, (me >> 1) & 3, (me & 1) ^ half
    around = [(z + step) & 3 for step in RING]
    bases = [(other * 2 + core) * SHARD for other in around]
    parts = [[(SHARD, (z * 2 + core) * SHARD)]]
    parts += [[(PART, base + PART * x) for base in bases], [(PART, base + 4 * PART + PART * y) for base in bases]]
    parts += [[(SHARD - 8 * PART, base + 8 * PART)] for base in bases]
    parts += [[(PART, base + PART * ((x + step) & 3)) for base in bases] for step in RING]
    parts += [[(PART, base + 4 * PART + PART * ((y + step) & 3)) for base in bases] for step in RING]
    return parts


def decode(me_ref, codes_ref, *refs):
    pieces, (out_ref, wide_ref, part_ref, staged_ref, sems) = refs[:-5], refs[-5:]
    me = me_ref[0]
    parts = table_parts(me, 0) + table_parts(me, 1)
    slots = part_ref.shape[0]
    work = []
    for piece, places in zip(pieces, parts):
        rows = piece.shape[0]
        if len(places) == 1:
            for at in range(0, rows, CHUNK):
                work.append((piece, at, min(CHUNK, rows - at), [(min(CHUNK, rows - at), places[0][1] + at)]))
        else:
            work.append((piece, 0, rows, places))

    def fetch(i):
        piece, at, rows, _ = work[i]
        return pltpu.make_async_copy(
            piece.at[pl.ds(at, rows)], part_ref.at[i % slots, pl.ds(0, rows)], sems.at[i % slots]
        )

    for i in range(slots):
        fetch(i).start()
    entries = wide_ref.shape[0] - 8
    wide_ref[pl.ds(entries, 8), :] = jnp.zeros((8, LANES), jnp.float32)
    for i, (_, _, _, places) in enumerate(work):
        fetch(i).wait()
        done = 0
        for rows, base in places:

            def widen(step, _, done=done, base=base, i=i):
                at = pl.multiple_of(done + step * LANES, LANES)
                to = pl.multiple_of(base + step * LANES, LANES)
                wide_ref[pl.ds(to, LANES), :] = part_ref[i % slots, pl.ds(at, LANES), :].astype(jnp.float32)
                return 0

            lax.fori_loop(0, rows // LANES, widen, 0)
            done += rows
        if i + slots < len(work):
            fetch(i + slots).start()

    def block(b, _):
        base = pl.multiple_of(b * LANES, LANES)
        for j in range(LANES):
            staged_ref[pl.ds(j, 1), :] = wide_ref[pl.ds(codes_ref[b, j], 1), :]
        out_ref[pl.ds(base, LANES), :] = staged_ref[...].astype(out_ref.dtype)
        return 0

    lax.fori_loop(0, BLOCKS, block, 0)


def moved(x, by):
    pairs = []
    for me in range(DEVICES):
        place = ((me >> 3) & 3, me >> 5, (me >> 1) & 3, me & 1)
        to_x, to_y, to_z, to_core = by(*place)
        pairs.append((me, ((to_y & 3) * 4 + (to_x & 3)) * 8 + (to_z & 3) * 2 + to_core))
    return lax.ppermute(x, ALL, pairs)


def along_x(piece):
    return [moved(piece, lambda x, y, z, core, step=step: (x - step, y, z, core)) for step in RING]


def along_y(piece):
    return [moved(piece, lambda x, y, z, core, step=step: (x, y - step, z, core)) for step in RING]


def along_z(piece):
    return [moved(piece, lambda x, y, z, core, step=step: (x, y, z - step, core)) for step in RING]


def other_core(piece):
    return moved(piece, lambda x, y, z, core: (x, y, z, 1 - core))


def first_pieces(table):
    row = lax.axis_index("rows")
    x, y = row & 3, row >> 2
    quarters = [
        lax.dynamic_slice_in_dim(table, PART * x, PART, 0),
        lax.dynamic_slice_in_dim(table, 4 * PART + PART * y, PART, 0),
    ]
    first = along_z(jnp.concatenate(quarters, axis=0))
    rest = along_z(table[8 * PART :])
    return first, rest


def later_pieces(first):
    for_x = jnp.concatenate([piece[:PART] for piece in first], axis=0)
    for_y = jnp.concatenate([piece[PART:] for piece in first], axis=0)
    return for_x, for_y, along_x(for_x), along_y(for_y)


def vmem():
    return pl.BlockSpec(memory_space=pltpu.VMEM)


def smem():
    return pl.BlockSpec(memory_space=pltpu.SMEM)


def exchange(x):
    return lax.all_to_all(x, ALL, 0, 0, tiled=True)


def steps(lookup_keys_per_record, filter_passed_flags, decoding_table):
    me = lax.axis_index(ALL).astype(jnp.int32).reshape(1)
    square = jax.ShapeDtypeStruct((DEVICES, LANES), jnp.int32)
    first, rest = first_pieces(decoding_table)
    other_table = other_core(decoding_table)
    sent = pl.pallas_call(local_compaction, out_shape=square, in_specs=[vmem(), vmem()], out_specs=vmem(), name="local_compaction")(
        lookup_keys_per_record.reshape(BLOCKS, LANES), filter_passed_flags.reshape(BLOCKS, LANES)
    )
    got = exchange(sent)
    for_x, for_y, from_x, from_y = later_pieces(first)
    other_xy = [other_core(for_x), other_core(for_y)]
    sent = pl.pallas_call(
        regroup,
        out_shape=square,
        in_specs=[smem(), smem(), vmem()],
        out_specs=vmem(),
        scratch_shapes=[pltpu.VMEM((DEVICES, LANES), jnp.int32)] * 2 + [pltpu.VMEM((DEVICES + 8, LANES), jnp.int32)],
        name="regroup",
    )(me, got[:, BLOCKS], got)
    got = exchange(sent)
    late = [*rest, *from_x, *from_y]
    other_late = [other_core(piece) for piece in late]
    pieces = [decoding_table, for_x, for_y, *late, other_table, *other_xy, *other_late]
    entries = 8 * SHARD
    codes = pl.pallas_call(
        functools.partial(placement, absent=entries),
        out_shape=jax.ShapeDtypeStruct((BLOCKS, LANES), jnp.int32),
        in_specs=[vmem()],
        out_specs=vmem(),
        name="placement",
    )(got)
    return pl.pallas_call(
        decode,
        out_shape=jax.ShapeDtypeStruct((BLOCKS * LANES, LANES), jnp.bfloat16),
        in_specs=[smem(), smem()] + [pl.BlockSpec(memory_space=pl.ANY)] * len(pieces),
        out_specs=vmem(),
        scratch_shapes=[
            pltpu.VMEM((entries + 8, LANES), jnp.float32),
            pltpu.VMEM((4, CHUNK, LANES), jnp.bfloat16),
            pltpu.VMEM((LANES, LANES), jnp.float32),
            pltpu.SemaphoreType.DMA((4,)),
        ],
        compiler_params=pltpu.CompilerParams(vmem_limit_bytes=48 << 20),
        name="decode",
    )(me, codes, *pieces)


def solution(mesh):
    placed = (P(ALL), P(ALL), P("dict", None))
    return jax.shard_map(steps, mesh=mesh, in_specs=placed, out_specs=P(ALL, None), check_vma=False)
```

```python
import jax
import jax.numpy as jnp
from jax import lax
from jax.experimental import pallas as pl
from jax.experimental.pallas import tpu as pltpu
from jax.sharding import PartitionSpec as P


ALL = ("rows", "dict")
LANES = 128
PRESENT = 1 << 30
DEVICES = 128
BLOCKS = 32
SHARD = 8192
PART = 768
HALF = PART // 2
REST = SHARD - 8 * PART
ENTRIES = 8 * SHARD
RING = (2, -1, 1)


def iota(shape, dim):
    return lax.broadcasted_iota(jnp.int32, shape, dim)


def exact_dot(a, b):
    return jnp.dot(a.astype(jnp.bfloat16), b.astype(jnp.bfloat16), preferred_element_type=jnp.float32)


def local_compaction(keys_ref, flags_ref, out_ref):
    flags = flags_ref[...]
    rows = flags.shape[0]
    upper = jnp.where(iota((LANES, LANES), 0) <= iota((LANES, LANES), 1), 1.0, 0.0)
    below = jnp.where(iota((rows, rows), 1) < iota((rows, rows), 0), 1.0, 0.0)
    kept = flags.astype(jnp.float32)
    inclusive = exact_dot(kept, upper)
    row_sums = exact_dot(kept, jnp.ones((LANES, LANES), jnp.float32))
    position = (inclusive + exact_dot(below, row_sums)).astype(jnp.int32) - 1
    count = jnp.sum(row_sums, axis=0, keepdims=True).astype(jnp.int32)
    here = iota((rows, LANES), 0) * LANES + iota((rows, LANES), 1)
    lane = iota((rows, LANES), 1)
    item = jnp.where(flags > 0, PRESENT | ((here - position) << 16) | keys_ref[...], 0)
    for level in range((rows * LANES - 1).bit_length()):
        step = 1 << level
        moving = (item >> (16 + level)) & 1 == 1
        sent = jnp.where(moving, item, 0)
        if step < LANES:
            near = pltpu.roll(sent, LANES - step, 1)
            arrived = jnp.where(lane < LANES - step, near, pltpu.roll(near, rows - 1, 0))
        else:
            arrived = pltpu.roll(sent, rows - step // LANES, 0)
        item = jnp.where(moving, 0, item) | arrived
    codes = item & 0xFFFF
    counts = jnp.broadcast_to(count, (LANES - rows, LANES))
    out_ref[...] = jnp.concatenate([codes, counts], axis=0).T


def regroup(me_ref, counts_ref, got_ref, out_ref, low_ref, high_ref, rows_ref):
    me = me_ref[0]
    got = got_ref[...]
    shape = got.shape
    lane = iota(shape, 1)
    count = jnp.max(jnp.where(lane >= BLOCKS, got, 0), axis=1, keepdims=True)
    count = jnp.broadcast_to(count, shape)
    below = jnp.where(iota(shape, 1) < iota(shape, 0), 1.0, 0.0)
    offset = 64 * exact_dot(below, (count >> 6).astype(jnp.float32)) + exact_dot(below, (count & 63).astype(jnp.float32))
    start = offset.astype(jnp.int32) + me
    valid = (lane < BLOCKS) & (lane * LANES + me < count)
    item = jnp.where(valid, PRESENT | ((start & 127) << 16) | got, 0)
    turn = (start >> 7) & (BLOCKS - 1)
    for level in range(5):
        item = jnp.where((turn >> level) & 1 == 1, pltpu.roll(item, 1 << level, 1), item)
    odd = iota(shape, 0) & 1 == 1
    low = jnp.where(lane < BLOCKS, item, 0)
    high = jnp.where(lane < BLOCKS, pltpu.roll(item, LANES - BLOCKS, 1), 0)
    low_ref[...] = jnp.where(odd, pltpu.roll(low, BLOCKS, 1), low)
    high_ref[...] = jnp.where(odd, pltpu.roll(high, BLOCKS, 1), high)
    rows_ref[...] = jnp.zeros_like(rows_ref)

    def place(s, before):
        d = (before + me) >> 12
        rows_ref[pl.ds(d, 1), :] = rows_ref[pl.ds(d, 1), :] | low_ref[pl.ds(s, 1), :]
        rows_ref[pl.ds(d + 1, 1), :] = rows_ref[pl.ds(d + 1, 1), :] | high_ref[pl.ds(s, 1), :]
        return before + counts_ref[s]

    lax.fori_loop(0, DEVICES, place, jnp.int32(0), unroll=8)
    out_ref[...] = rows_ref[:DEVICES, :]


def colours(x, y):
    return (x + 2 * y) & 3, (2 * x + y) & 3


def table_parts(me, half):
    x, y, z, core = (me >> 3) & 3, me >> 5, (me >> 1) & 3, (me & 1) ^ half
    a, b = colours(x, y)
    bases = [(((z + step) & 3) * 2 + core) * SHARD for step in RING]

    def first(colour, at=0):
        return PART * (colour & 3) + at

    def second(colour, at=0):
        return PART * (4 + (colour & 3)) + at

    def pieces(whole, part):
        return [(PART, base + whole) for base in bases] + [(HALF, base + part) for base in bases]

    parts = [[(SHARD, (z * 2 + core) * SHARD)]]
    parts += [[(PART, base + at) for base in bases for at in (first(a), second(b))]]
    parts += [[(REST, base + 8 * PART)] for base in bases]
    parts += [pieces(first(a - 1), second(b + 2)), pieces(first(a + 1), second(b + 2, HALF))]
    parts += [pieces(second(b - 1), first(a + 2)), pieces(second(b + 1), first(a + 2, HALF))]
    return parts


def decode(me_ref, got_ref, *refs):
    pieces, (out_ref, table_ref, pairs_ref, wide_ref, place_ref, scalar_ref, sem, place_sem) = refs[:-8], refs[-8:]
    me = me_ref[0]
    for piece, places in zip(pieces, table_parts(me, 0) + table_parts(me, 1)):
        at = 0
        for rows, base in places:
            pltpu.make_async_copy(
                piece.at[pl.ds(at // 2, rows // 2)], table_ref.at[pl.ds(base >> 1, rows // 2)], sem
            ).start()
            at += rows
    table_ref[pl.ds(ENTRIES // 2, 8)] = jnp.zeros((8, 2, LANES), table_ref.dtype)

    item = got_ref[...].T[: 2 * BLOCKS]
    lane = iota(item.shape, 1)
    turn = (((item >> 16) & 127) - lane) & 127
    item = jnp.where(item > 0, (item & (PRESENT | 0xFFFF)) | (turn << 16), 0)
    for level in range(7):
        moving = (item >> (16 + level)) & 1 == 1
        item = jnp.where(moving, 0, item) | pltpu.roll(jnp.where(moving, item, 0), 1 << level, 1)
    item = item[:BLOCKS] | item[BLOCKS:]
    place_ref[...] = jnp.where(item > 0, (item & 0xFFFF) >> 1, ENTRIES // 2)
    to_scalars = pltpu.make_async_copy(place_ref, scalar_ref, place_sem)
    to_scalars.start()
    odd = jnp.concatenate([item & 1, jnp.zeros((LANES - BLOCKS, LANES), jnp.int32)], axis=0).T
    to_scalars.wait()
    filled = table_ref.at[pl.ds(0, ENTRIES // 2)]
    pltpu.make_async_copy(filled, filled, sem).wait()

    def fetch(b, _):
        for j in range(LANES):
            pairs_ref[b, 2 * j : 2 * j + 2, :] = table_ref[scalar_ref[b, j]]
        return 0

    lax.fori_loop(0, BLOCKS, fetch, 0)
    for b in range(BLOCKS):
        wide = wide_ref.at[b % 4]
        wide[...] = pairs_ref[b].astype(jnp.float32)
        second = jnp.broadcast_to(odd[:, b : b + 1], (LANES, LANES)) == 1
        row = jnp.where(second, wide[pl.ds(1, LANES, stride=2), :], wide[pl.ds(0, LANES, stride=2), :])
        out_ref[b * LANES : (b + 1) * LANES, :] = row.astype(out_ref.dtype)


def moved(x, by):
    pairs = []
    for me in range(DEVICES):
        place = ((me >> 3) & 3, me >> 5, (me >> 1) & 3, me & 1)
        to_x, to_y, to_z, to_core = by(*place)
        pairs.append((me, ((to_y & 3) * 4 + (to_x & 3)) * 8 + (to_z & 3) * 2 + to_core))
    return lax.ppermute(x, ALL, pairs)


def along_z(piece):
    return [moved(piece, lambda x, y, z, core, step=step: (x, y, z - step, core)) for step in RING]


def other_core(piece):
    return moved(piece, lambda x, y, z, core: (x, y, z, 1 - core))


def cut(me_ref, table_ref, parts_ref, rest_ref, sems):
    a, b = colours((me_ref[0] >> 3) & 3, me_ref[0] >> 5)
    copies = [
        pltpu.make_async_copy(table_ref.at[pl.ds(PART * a, PART)], parts_ref.at[pl.ds(0, PART)], sems.at[0]),
        pltpu.make_async_copy(table_ref.at[pl.ds(PART * (4 + b), PART)], parts_ref.at[pl.ds(PART, PART)], sems.at[1]),
        pltpu.make_async_copy(table_ref.at[pl.ds(8 * PART, REST)], rest_ref, sems.at[2]),
    ]
    for copy in copies:
        copy.start()
    for copy in copies:
        copy.wait()


def join(*refs):
    pieces, joined, all_ref = refs[: len(RING)], refs[len(RING) : -1], refs[-1]
    for out, (whole, part) in zip(joined, ((0, PART), (0, PART + HALF), (PART, 0), (PART, HALF))):
        for k, piece in enumerate(pieces):
            out[PART * k : PART * (k + 1), :] = piece[whole : whole + PART, :]
            to = PART * len(RING) + HALF * k
            out[to : to + HALF, :] = piece[part : part + HALF, :]
    for k, piece in enumerate(pieces):
        all_ref[2 * PART * k : 2 * PART * (k + 1), :] = piece[...]


def first_pieces(me, table):
    parts, rest = pl.pallas_call(
        cut,
        out_shape=[pltpu.VMEM((rows, LANES), table.dtype) for rows in (2 * PART, REST)],
        in_specs=[smem(), anywhere()],
        out_specs=[vmem()] * 2,
        scratch_shapes=[pltpu.SemaphoreType.DMA((3,))],
        name="cut",
    )(me, table)
    first = along_z(parts)
    rest = along_z(rest)
    return first, rest


def ring_pieces(first):
    rows = len(RING) * (PART + HALF)
    *sent, every = pl.pallas_call(
        join,
        out_shape=[pltpu.VMEM((rows, LANES), first[0].dtype)] * 4
        + [jax.ShapeDtypeStruct((2 * PART * len(RING), LANES), first[0].dtype)],
        in_specs=[vmem()] * len(first),
        out_specs=[vmem()] * 5,
        name="join",
    )(*first)
    return every, [
        moved(sent[0], lambda x, y, z, core: (x + 1, y, z, core)),
        moved(sent[1], lambda x, y, z, core: (x - 1, y, z, core)),
        moved(sent[2], lambda x, y, z, core: (x, y + 1, z, core)),
        moved(sent[3], lambda x, y, z, core: (x, y - 1, z, core)),
    ]


def anywhere():
    return pl.BlockSpec(memory_space=pl.ANY)


def vmem():
    return pl.BlockSpec(memory_space=pltpu.VMEM)


def smem():
    return pl.BlockSpec(memory_space=pltpu.SMEM)


def exchange(x):
    return lax.all_to_all(x, ALL, 0, 0, tiled=True)


def steps(lookup_keys_per_record, filter_passed_flags, decoding_table):
    me = lax.axis_index(ALL).astype(jnp.int32).reshape(1)
    square = jax.ShapeDtypeStruct((DEVICES, LANES), jnp.int32)
    first, rest = first_pieces(me, decoding_table)
    other_table = other_core(decoding_table)
    sent = pl.pallas_call(local_compaction, out_shape=square, in_specs=[vmem(), vmem()], out_specs=vmem(), name="local_compaction")(
        lookup_keys_per_record.reshape(BLOCKS, LANES), filter_passed_flags.reshape(BLOCKS, LANES)
    )
    got = exchange(sent)
    every, ring = ring_pieces(first)
    other_every = other_core(every)
    sent = pl.pallas_call(
        regroup,
        out_shape=square,
        in_specs=[smem(), smem(), vmem()],
        out_specs=vmem(),
        scratch_shapes=[pltpu.VMEM((DEVICES, LANES), jnp.int32)] * 2 + [pltpu.VMEM((DEVICES + 8, LANES), jnp.int32)],
        name="regroup",
    )(me, got[:, BLOCKS], got)
    got = exchange(sent)
    other_rest = [other_core(piece) for piece in rest]
    other_ring = [other_core(piece) for piece in ring]
    pieces = [decoding_table, every, *rest, *ring, other_table, other_every, *other_rest, *other_ring]
    pieces = [pltpu.with_memory_space_constraint(piece.reshape(-1, 2, LANES), pltpu.HBM) for piece in pieces]
    return pl.pallas_call(
        decode,
        out_shape=jax.ShapeDtypeStruct((BLOCKS * LANES, LANES), jnp.bfloat16),
        in_specs=[smem(), vmem()] + [anywhere()] * len(pieces),
        out_specs=vmem(),
        scratch_shapes=[
            pltpu.VMEM((ENTRIES // 2 + 8, 2, LANES), jnp.bfloat16),
            pltpu.VMEM((BLOCKS, 2 * LANES, LANES), jnp.bfloat16),
            pltpu.VMEM((4, 2 * LANES, LANES), jnp.float32),
            pltpu.VMEM((BLOCKS, LANES), jnp.int32),
            pltpu.SMEM((BLOCKS, LANES), jnp.int32),
            pltpu.SemaphoreType.DMA(()),
            pltpu.SemaphoreType.DMA(()),
        ],
        compiler_params=pltpu.CompilerParams(vmem_limit_bytes=32 << 20),
        name="decode",
    )(me, got, *pieces)


def solution(mesh):
    placed = (P(ALL), P(ALL), P("dict", None))
    return jax.shard_map(steps, mesh=mesh, in_specs=placed, out_specs=P(ALL, None), check_vma=False)
```

```python
import jax
import jax.numpy as jnp
from jax import lax
from jax.experimental import pallas as pl
from jax.experimental.pallas import tpu as pltpu
from jax.sharding import PartitionSpec as P


ALL = ("rows", "dict")
LANES = 128
PRESENT = 1 << 23
DEVICES = 128
BLOCKS = 32
SHARD = 8192
RING = (2, -1, 1)
LARGE, SMALLER = (1216, 672, 672), (832, 480, 480)
BOTH = tuple(large + smaller for large, smaller in zip(LARGE, SMALLER))
REST = SHARD - 4 * BOTH[1]
ENTRIES = 8 * SHARD
SMALL = pltpu.CompilerParams(vmem_limit_bytes=8 << 20)


def iota(shape, dim):
    return lax.broadcasted_iota(jnp.int32, shape, dim)


def exact_dot(a, b):
    return jnp.dot(a.astype(jnp.bfloat16), b.astype(jnp.bfloat16), preferred_element_type=jnp.float32)


def local_compaction(keys_ref, flags_ref, out_ref):
    flags = flags_ref[...]
    rows = flags.shape[0]
    upper = jnp.where(iota((LANES, LANES), 0) <= iota((LANES, LANES), 1), 1.0, 0.0)
    below = jnp.where(iota((rows, rows), 1) < iota((rows, rows), 0), 1.0, 0.0)
    kept = flags.astype(jnp.float32)
    inclusive = exact_dot(kept, upper)
    row_sums = exact_dot(kept, jnp.ones((LANES, LANES), jnp.float32))
    position = (inclusive + exact_dot(below, row_sums)).astype(jnp.int32) - 1
    count = jnp.sum(row_sums, axis=0, keepdims=True).astype(jnp.int32)
    here = iota((rows, LANES), 0) * LANES + iota((rows, LANES), 1)
    lane = iota((rows, LANES), 1)
    item = jnp.where(flags > 0, ((here - position) << 16) | keys_ref[...], 0)
    for level in range((rows * LANES - 1).bit_length()):
        step = 1 << level
        moving = (item >> (16 + level)) & 1 == 1
        sent = jnp.where(moving, item, 0)
        if step < LANES:
            near = pltpu.roll(sent, LANES - step, 1)
            arrived = jnp.where(lane < LANES - step, near, pltpu.roll(near, rows - 1, 0))
        else:
            arrived = pltpu.roll(sent, rows - step // LANES, 0)
        item = jnp.where(moving, 0, item) | arrived
    codes = item & 0xFFFF
    counts = jnp.broadcast_to(count, (LANES - rows, LANES))
    out_ref[...] = jnp.concatenate([codes, counts], axis=0).T


def regroup(me_ref, got_ref, out_ref):
    me = me_ref[0]
    got = got_ref[...]
    shape = got.shape
    lane = iota(shape, 1)
    count = jnp.max(jnp.where(lane >= BLOCKS, got, 0), axis=1, keepdims=True)
    count = jnp.broadcast_to(count, shape)
    below = jnp.where(iota(shape, 1) < iota(shape, 0), 1.0, 0.0)
    offset = 64 * exact_dot(below, (count >> 6).astype(jnp.float32)) + exact_dot(below, (count & 63).astype(jnp.float32))
    start = offset.astype(jnp.int32) + me
    valid = (lane < BLOCKS) & (lane * LANES + me < count)
    item = jnp.where(valid, PRESENT | ((start & 127) << 16) | got, 0)
    turn = (start >> 7) & (BLOCKS - 1)
    for level in range(5):
        item = jnp.where((turn >> level) & 1 == 1, pltpu.roll(item, 1 << level, 1), item)
    odd = iota(shape, 0) & 1 == 1
    low = jnp.where(lane < BLOCKS, item, 0)
    high = jnp.where(lane < BLOCKS, pltpu.roll(item, LANES - BLOCKS, 1), 0)
    low = jnp.where(odd, pltpu.roll(low, BLOCKS, 1), low)
    high = jnp.where(odd, pltpu.roll(high, BLOCKS, 1), high)
    both = jnp.concatenate([low, high], axis=0)
    device = (start >> 12).T
    here = iota(shape, 0)
    chosen = [jnp.where(device + next_one == here, 1.0, 0.0) for next_one in (0, 1)]
    chosen = jnp.concatenate(chosen, axis=1)
    total = exact_dot(chosen, (both & 255).astype(jnp.float32))
    total += 256 * exact_dot(chosen, ((both >> 8) & 255).astype(jnp.float32))
    total += 65536 * exact_dot(chosen, (both >> 16).astype(jnp.float32))
    out_ref[...] = total.astype(jnp.int32)


def colours(x, y):
    return (x + 2 * y) & 3, (2 * x + y) & 3


def table_parts(me, half):
    x, y, z, core = (me >> 3) & 3, me >> 5, (me >> 1) & 3, (me & 1) ^ half
    a, b = colours(x, y)
    bases = [(((z + step) & 3) * 2 + core) * SHARD for step in RING]
    a_rows = list(zip(LARGE, bases))
    b_rows = list(zip(SMALLER, [base + 4 * rows for rows, base in a_rows]))

    def whole(parts, colour):
        return [(rows, base + rows * (colour & 3)) for rows, base in parts]

    def part(parts, colour, at):
        return [(rows // 2, base + rows * (colour & 3) + at * (rows // 2)) for rows, base in parts]

    places = [[(SHARD, (z * 2 + core) * SHARD)]]
    places += [[place for pair in zip(whole(a_rows, a), whole(b_rows, b)) for place in pair]]
    places += [[(REST, base + SHARD - REST)] for base in bases[1:]]
    places += [whole(a_rows, a - 1) + part(b_rows, b + 2, 0), whole(a_rows, a + 1) + part(b_rows, b + 2, 1)]
    places += [whole(b_rows, b - 1) + part(a_rows, a + 2, 0), whole(b_rows, b + 1) + part(a_rows, a + 2, 1)]
    return places


def decode(me_ref, got_ref, *refs):
    pieces, (out_ref, table_ref, pairs_ref, wide_ref, place_ref, scalar_ref, sem, place_sem) = refs[:-8], refs[-8:]
    me = me_ref[0]
    for piece, places in zip(pieces, table_parts(me, 0) + table_parts(me, 1)):
        at = 0
        for rows, base in places:
            pltpu.make_async_copy(
                piece.at[pl.ds(at // 2, rows // 2)], table_ref.at[pl.ds(base >> 1, rows // 2)], sem
            ).start()
            at += rows
    table_ref[pl.ds(ENTRIES // 2, 8)] = jnp.zeros((8, 2, LANES), table_ref.dtype)

    item = got_ref[...].T[: 2 * BLOCKS]
    lane = iota(item.shape, 1)
    turn = (((item >> 16) & 127) - lane) & 127
    item = jnp.where(item > 0, (item & (PRESENT | 0xFFFF)) | (turn << 16), 0)
    for level in range(7):
        moving = (item >> (16 + level)) & 1 == 1
        item = jnp.where(moving, 0, item) | pltpu.roll(jnp.where(moving, item, 0), 1 << level, 1)
    item = item[:BLOCKS] | item[BLOCKS:]
    place_ref[...] = jnp.where(item > 0, (item & 0xFFFF) >> 1, ENTRIES // 2)
    to_scalars = pltpu.make_async_copy(place_ref, scalar_ref, place_sem)
    to_scalars.start()
    odd = jnp.concatenate([item & 1, jnp.zeros((LANES - BLOCKS, LANES), jnp.int32)], axis=0).T
    to_scalars.wait()
    filled = table_ref.at[pl.ds(0, ENTRIES // 2)]
    pltpu.make_async_copy(filled, filled, sem).wait()

    def fetch(b, _):
        for j in range(LANES):
            pairs_ref[b, 2 * j : 2 * j + 2, :] = table_ref[scalar_ref[b, j]]
        return 0

    lax.fori_loop(0, BLOCKS, fetch, 0)
    for b in range(BLOCKS):
        wide = wide_ref.at[b % 4]
        wide[...] = pairs_ref[b].astype(jnp.float32)
        second = jnp.broadcast_to(odd[:, b : b + 1], (LANES, LANES)) == 1
        row = jnp.where(second, wide[pl.ds(1, LANES, stride=2), :], wide[pl.ds(0, LANES, stride=2), :])
        out_ref[b * LANES : (b + 1) * LANES, :] = row.astype(out_ref.dtype)


def moved(x, by):
    pairs = []
    for me in range(DEVICES):
        place = ((me >> 3) & 3, me >> 5, (me >> 1) & 3, me & 1)
        to_x, to_y, to_z, to_core = by(*place)
        pairs.append((me, ((to_y & 3) * 4 + (to_x & 3)) * 8 + (to_z & 3) * 2 + to_core))
    return lax.ppermute(x, ALL, pairs)


def along_z(pieces, steps):
    return [
        moved(piece, lambda x, y, z, core, step=step: (x, y, z - step, core)) for piece, step in zip(pieces, steps)
    ]


def other_core(piece):
    return moved(piece, lambda x, y, z, core: (x, y, z, 1 - core))


def cut(me_ref, table_ref, far_ref, near_ref, sems):
    a, b = colours((me_ref[0] >> 3) & 3, me_ref[0] >> 5)
    copies = []
    for out, large, smaller in ((far_ref, LARGE[0], SMALLER[0]), (near_ref, LARGE[1], SMALLER[1])):
        for at, to, rows in ((large * a, 0, large), (4 * large + smaller * b, large, smaller)):
            copies.append(
                pltpu.make_async_copy(table_ref.at[pl.ds(at, rows)], out.at[pl.ds(to, rows)], sems.at[len(copies)])
            )
    for copy in copies:
        copy.start()
    for copy in copies:
        copy.wait()


def join(*refs):
    pieces, joined, all_ref = refs[: len(RING)], refs[len(RING) : -1], refs[-1]
    for number, out in enumerate(joined):
        to = 0
        for share in (1, 2):
            for large, smaller, piece in zip(LARGE, SMALLER, pieces):
                begin, rows = (0, large) if (number < 2) == (share == 1) else (large, smaller)
                rows //= share
                begin += rows * (number % 2) * (share - 1)
                out[to : to + rows, :] = piece[begin : begin + rows, :]
                to += rows
    to = 0
    for rows, piece in zip(BOTH, pieces):
        all_ref[to : to + rows, :] = piece[...]
        to += rows


def first_pieces(me, table):
    far, near = pl.pallas_call(
        cut,
        out_shape=[pltpu.VMEM((rows, LANES), table.dtype) for rows in BOTH[:2]],
        in_specs=[smem(), anywhere()],
        out_specs=[vmem()] * 2,
        scratch_shapes=[pltpu.SemaphoreType.DMA((4,))],
        name="cut",
    )(me, pltpu.with_memory_space_constraint(table, pltpu.HBM))
    first = along_z([far, near, near], RING)
    rest = along_z([table[SHARD - REST :]] * 2, RING[1:])
    return first, rest


def ring_pieces(first):
    rows = [sum(LARGE) + sum(SMALLER) // 2] * 2 + [sum(SMALLER) + sum(LARGE) // 2] * 2
    *sent, every = pl.pallas_call(
        join,
        out_shape=[pltpu.VMEM((count, LANES), first[0].dtype) for count in rows]
        + [jax.ShapeDtypeStruct((sum(BOTH), LANES), first[0].dtype)],
        in_specs=[vmem()] * len(first),
        out_specs=[vmem()] * 5,
        compiler_params=SMALL,
        name="join",
    )(*first)
    ring = [
        moved(sent[0], lambda x, y, z, core: (x + 1, y, z, core)),
        moved(sent[1], lambda x, y, z, core: (x - 1, y, z, core)),
    ]
    ring += [
        moved(sent[2], lambda x, y, z, core: (x, y + 1, z, core)),
        moved(sent[3], lambda x, y, z, core: (x, y - 1, z, core)),
    ]
    return every, ring


def anywhere():
    return pl.BlockSpec(memory_space=pl.ANY)


def vmem():
    return pl.BlockSpec(memory_space=pltpu.VMEM)


def smem():
    return pl.BlockSpec(memory_space=pltpu.SMEM)


def exchange(x):
    return lax.all_to_all(x, ALL, 0, 0, tiled=True)


def steps(lookup_keys_per_record, filter_passed_flags, decoding_table):
    me = lax.axis_index(ALL).astype(jnp.int32).reshape(1)
    square = jax.ShapeDtypeStruct((DEVICES, LANES), jnp.int32)
    first, rest = first_pieces(me, decoding_table)
    other_table = other_core(decoding_table)
    sent = pl.pallas_call(local_compaction, out_shape=square, in_specs=[vmem(), vmem()], out_specs=vmem(), compiler_params=SMALL, name="local_compaction")(
        lookup_keys_per_record.reshape(BLOCKS, LANES), filter_passed_flags.reshape(BLOCKS, LANES)
    )
    got = exchange(sent)
    every, ring = ring_pieces(first)
    other_every = other_core(every)
    sent = pl.pallas_call(
        regroup,
        out_shape=square,
        in_specs=[smem(), vmem()],
        out_specs=vmem(),
        compiler_params=SMALL,
        name="regroup",
    )(me, got)
    got = exchange(sent)
    other_rest = [other_core(piece) for piece in rest]
    other_ring = [other_core(piece) for piece in ring[:2]]
    other_ring += [other_core(piece) for piece in ring[2:]]
    pieces = [decoding_table, every, *rest, *ring, other_table, other_every, *other_rest, *other_ring]
    pieces = [pltpu.with_memory_space_constraint(piece.reshape(-1, 2, LANES), pltpu.HBM) for piece in pieces]
    return pl.pallas_call(
        decode,
        out_shape=jax.ShapeDtypeStruct((BLOCKS * LANES, LANES), jnp.bfloat16),
        in_specs=[smem(), vmem()] + [anywhere()] * len(pieces),
        out_specs=vmem(),
        scratch_shapes=[
            pltpu.VMEM((ENTRIES // 2 + 8, 2, LANES), jnp.bfloat16),
            pltpu.VMEM((BLOCKS, 2 * LANES, LANES), jnp.bfloat16),
            pltpu.VMEM((4, 2 * LANES, LANES), jnp.float32),
            pltpu.VMEM((BLOCKS, LANES), jnp.int32),
            pltpu.SMEM((BLOCKS, LANES), jnp.int32),
            pltpu.SemaphoreType.DMA(()),
            pltpu.SemaphoreType.DMA(()),
        ],
        compiler_params=pltpu.CompilerParams(vmem_limit_bytes=32 << 20),
        name="decode",
    )(me, got, *pieces)


def solution(mesh):
    placed = (P(ALL), P(ALL), P("dict", None))
    return jax.shard_map(steps, mesh=mesh, in_specs=placed, out_specs=P(ALL, None), check_vma=False)
```

```python
import jax
import jax.numpy as jnp
from jax import lax
from jax.experimental import pallas as pl
from jax.experimental.pallas import tpu as pltpu
from jax.sharding import PartitionSpec as P


ALL = ("rows", "dict")
LANES = 128
PRESENT = 1 << 23
DEVICES = 128
BLOCKS = 32
SHARD = 8192
RING = (2, -1, 1)
LARGE, SMALLER = (1216, 640, 640), (832, 448, 448)
BOTH = tuple(large + smaller for large, smaller in zip(LARGE, SMALLER))
REST = SHARD - 4 * BOTH[1]
ENTRIES = 8 * SHARD
HELD = 8192
SMALL = pltpu.CompilerParams(vmem_limit_bytes=8 << 20)


def iota(shape, dim):
    return lax.broadcasted_iota(jnp.int32, shape, dim)


def exact_dot(a, b):
    return jnp.dot(a.astype(jnp.bfloat16), b.astype(jnp.bfloat16), preferred_element_type=jnp.float32)


def local_compaction(keys_ref, flags_ref, out_ref):
    flags = flags_ref[...]
    rows = flags.shape[0]
    upper = jnp.where(iota((LANES, LANES), 0) <= iota((LANES, LANES), 1), 1.0, 0.0)
    below = jnp.where(iota((rows, rows), 1) < iota((rows, rows), 0), 1.0, 0.0)
    kept = flags.astype(jnp.float32)
    inclusive = exact_dot(kept, upper)
    row_sums = exact_dot(kept, jnp.ones((LANES, LANES), jnp.float32))
    position = (inclusive + exact_dot(below, row_sums)).astype(jnp.int32) - 1
    count = jnp.sum(row_sums, axis=0, keepdims=True).astype(jnp.int32)
    here = iota((rows, LANES), 0) * LANES + iota((rows, LANES), 1)
    lane = iota((rows, LANES), 1)
    item = jnp.where(flags > 0, ((here - position) << 16) | keys_ref[...], 0)
    for level in range((rows * LANES - 1).bit_length()):
        step = 1 << level
        moving = (item >> (16 + level)) & 1 == 1
        sent = jnp.where(moving, item, 0)
        if step < LANES:
            near = pltpu.roll(sent, LANES - step, 1)
            arrived = jnp.where(lane < LANES - step, near, pltpu.roll(near, rows - 1, 0))
        else:
            arrived = pltpu.roll(sent, rows - step // LANES, 0)
        item = jnp.where(moving, 0, item) | arrived
    codes = item & 0xFFFF
    counts = jnp.broadcast_to(count, (LANES - rows, LANES))
    out_ref[...] = jnp.concatenate([codes, counts], axis=0).T


def regroup(me_ref, got_ref, out_ref):
    me = me_ref[0]
    got = got_ref[...]
    shape = got.shape
    lane = iota(shape, 1)
    count = jnp.max(jnp.where(lane >= BLOCKS, got, 0), axis=1, keepdims=True)
    count = jnp.broadcast_to(count, shape)
    below = jnp.where(iota(shape, 1) < iota(shape, 0), 1.0, 0.0)
    offset = 64 * exact_dot(below, (count >> 6).astype(jnp.float32)) + exact_dot(below, (count & 63).astype(jnp.float32))
    start = offset.astype(jnp.int32) + me
    valid = (lane < BLOCKS) & (lane * LANES + me < count)
    item = jnp.where(valid, PRESENT | ((start & 127) << 16) | got, 0)
    turn = (start >> 7) & (BLOCKS - 1)
    for level in range(5):
        item = jnp.where((turn >> level) & 1 == 1, pltpu.roll(item, 1 << level, 1), item)
    odd = iota(shape, 0) & 1 == 1
    low = jnp.where(lane < BLOCKS, item, 0)
    high = jnp.where(lane < BLOCKS, pltpu.roll(item, LANES - BLOCKS, 1), 0)
    low = jnp.where(odd, pltpu.roll(low, BLOCKS, 1), low)
    high = jnp.where(odd, pltpu.roll(high, BLOCKS, 1), high)
    both = jnp.concatenate([low, high], axis=0)
    device = (start >> 12).T
    here = iota(shape, 0)
    chosen = [jnp.where(device + next_one == here, 1.0, 0.0) for next_one in (0, 1)]
    chosen = jnp.concatenate(chosen, axis=1)
    total = exact_dot(chosen, (both & 255).astype(jnp.float32))
    total += 256 * exact_dot(chosen, ((both >> 8) & 255).astype(jnp.float32))
    total += 65536 * exact_dot(chosen, (both >> 16).astype(jnp.float32))
    out_ref[...] = total.astype(jnp.int32)


def colours(x, y):
    return (x + 2 * y) & 3, (2 * x + y) & 3


def table_parts(me, half):
    x, y, z, core = (me >> 3) & 3, me >> 5, (me >> 1) & 3, (me & 1) ^ half
    a, b = colours(x, y)
    bases = [(((z + step) & 3) * 2 + core) * SHARD for step in RING]
    a_rows = list(zip(LARGE, bases))
    b_rows = list(zip(SMALLER, [base + 4 * rows for rows, base in a_rows]))

    def whole(parts, colour):
        return [(rows, base + rows * (colour & 3)) for rows, base in parts]

    def part(parts, colour, at):
        return [(rows // 2, base + rows * (colour & 3) + at * (rows // 2)) for rows, base in parts]

    places = [[(SHARD, (z * 2 + core) * SHARD)]]
    places += [[place for pair in zip(whole(a_rows, a), whole(b_rows, b)) for place in pair]]
    places += [[(REST, base + SHARD - REST)] for base in bases[1:]]
    places += [whole(a_rows, a - 1) + part(b_rows, b + 2, 0), whole(a_rows, a + 1) + part(b_rows, b + 2, 1)]
    places += [whole(b_rows, b - 1) + part(a_rows, a + 2, 0), whole(b_rows, b + 1) + part(a_rows, a + 2, 1)]
    return places


def decode(me_ref, got_ref, held_ref, *refs):
    pieces, (out_ref, table_ref, pairs_ref, wide_ref, place_ref, scalar_ref, sem, place_sem) = refs[:-8], refs[-8:]
    me = me_ref[0]
    for piece, places in zip(pieces, table_parts(me, 0) + table_parts(me, 1)):
        at = 0
        for rows, base in places:
            pltpu.make_async_copy(
                piece.at[pl.ds(at // 2, rows // 2)], table_ref.at[pl.ds(base >> 1, rows // 2)], sem
            ).start()
            at += rows
    table_ref[pl.ds(ENTRIES // 2, 8)] = jnp.zeros((8, 2, LANES), table_ref.dtype)

    item = got_ref[...].T[: 2 * BLOCKS]
    lane = iota(item.shape, 1)
    turn = (((item >> 16) & 127) - lane) & 127
    item = jnp.where(item > 0, (item & (PRESENT | 0xFFFF)) | (turn << 16), 0)
    for level in range(7):
        moving = (item >> (16 + level)) & 1 == 1
        item = jnp.where(moving, 0, item) | pltpu.roll(jnp.where(moving, item, 0), 1 << level, 1)
    item = item[:BLOCKS] | item[BLOCKS:]
    place_ref[...] = jnp.where(item > 0, (item & 0xFFFF) >> 1, ENTRIES // 2)
    to_scalars = pltpu.make_async_copy(place_ref, scalar_ref, place_sem)
    to_scalars.start()
    odd = jnp.concatenate([item & 1, jnp.zeros((LANES - BLOCKS, LANES), jnp.int32)], axis=0).T
    to_scalars.wait()
    filled = table_ref.at[pl.ds(0, ENTRIES // 2)]
    pltpu.make_async_copy(filled, filled, sem).wait()

    def fetch(b, _):
        for j in range(LANES):
            pairs_ref[b, 2 * j : 2 * j + 2, :] = table_ref[scalar_ref[b, j]]
        return 0

    lax.fori_loop(0, BLOCKS, fetch, 0)
    for b in range(BLOCKS):
        wide = wide_ref.at[b % 4]
        wide[...] = pairs_ref[b].astype(jnp.float32)
        second = jnp.broadcast_to(odd[:, b : b + 1], (LANES, LANES)) == 1
        row = jnp.where(second, wide[pl.ds(1, LANES, stride=2), :], wide[pl.ds(0, LANES, stride=2), :])
        out_ref[b * LANES : (b + 1) * LANES, :] = row.astype(out_ref.dtype)


def moved(x, by):
    pairs = []
    for me in range(DEVICES):
        place = ((me >> 3) & 3, me >> 5, (me >> 1) & 3, me & 1)
        to_x, to_y, to_z, to_core = by(*place)
        pairs.append((me, ((to_y & 3) * 4 + (to_x & 3)) * 8 + (to_z & 3) * 2 + to_core))
    return lax.ppermute(x, ALL, pairs)


def along_z(pieces, steps):
    return [
        moved(piece, lambda x, y, z, core, step=step: (x, y, z - step, core)) for piece, step in zip(pieces, steps)
    ]


def other_core(piece):
    return moved(piece, lambda x, y, z, core: (x, y, z, 1 - core))


def cut(me_ref, table_ref, far_ref, near_ref, sems):
    a, b = colours((me_ref[0] >> 3) & 3, me_ref[0] >> 5)
    copies = []
    for out, large, smaller in ((far_ref, LARGE[0], SMALLER[0]), (near_ref, LARGE[1], SMALLER[1])):
        for at, to, rows in ((large * a, 0, large), (4 * large + smaller * b, large, smaller)):
            copies.append(
                pltpu.make_async_copy(table_ref.at[pl.ds(at, rows)], out.at[pl.ds(to, rows)], sems.at[len(copies)])
            )
    for copy in copies:
        copy.start()
    for copy in copies:
        copy.wait()


def join(*refs):
    pieces, joined, all_ref = refs[: len(RING)], refs[len(RING) : -1], refs[-1]
    for number, out in enumerate(joined):
        to = 0
        for share in (1, 2):
            for large, smaller, piece in zip(LARGE, SMALLER, pieces):
                begin, rows = (0, large) if (number < 2) == (share == 1) else (large, smaller)
                rows //= share
                begin += rows * (number % 2) * (share - 1)
                out[to : to + rows, :] = piece[begin : begin + rows, :]
                to += rows
    to = 0
    for rows, piece in zip(BOTH, pieces):
        all_ref[to : to + rows, :] = piece[...]
        to += rows


def first_pieces(me, table):
    far, near = pl.pallas_call(
        cut,
        out_shape=[pltpu.VMEM((rows, LANES), table.dtype) for rows in BOTH[:2]],
        in_specs=[smem(), anywhere()],
        out_specs=[vmem()] * 2,
        scratch_shapes=[pltpu.SemaphoreType.DMA((4,))],
        name="cut",
    )(me, pltpu.with_memory_space_constraint(table, pltpu.HBM))
    first = along_z([far, near, near], RING)
    rest = along_z([table[SHARD - REST :]] * 2, RING[1:])
    return first, rest


def ring_pieces(first):
    rows = [sum(LARGE) + sum(SMALLER) // 2] * 2 + [sum(SMALLER) + sum(LARGE) // 2] * 2
    *sent, every = pl.pallas_call(
        join,
        out_shape=[pltpu.VMEM((count, LANES), first[0].dtype) for count in rows]
        + [jax.ShapeDtypeStruct((sum(BOTH), LANES), first[0].dtype)],
        in_specs=[vmem()] * len(first),
        out_specs=[vmem()] * 5,
        compiler_params=SMALL,
        name="join",
    )(*first)
    ring = [
        moved(sent[0], lambda x, y, z, core: (x + 1, y, z, core)),
        moved(sent[1], lambda x, y, z, core: (x - 1, y, z, core)),
    ]
    ring += [
        moved(sent[2], lambda x, y, z, core: (x, y + 1, z, core)),
        moved(sent[3], lambda x, y, z, core: (x, y - 1, z, core)),
    ]
    return every, ring


def anywhere():
    return pl.BlockSpec(memory_space=pl.ANY)


def hold(me_ref, held_ref):
    held_ref[:16, :] = jnp.zeros((16, LANES), held_ref.dtype)


def vmem():
    return pl.BlockSpec(memory_space=pltpu.VMEM)


def smem():
    return pl.BlockSpec(memory_space=pltpu.SMEM)


def exchange(x):
    return lax.all_to_all(x, ALL, 0, 0, tiled=True)


def steps(lookup_keys_per_record, filter_passed_flags, decoding_table):
    me = lax.axis_index(ALL).astype(jnp.int32).reshape(1)
    square = jax.ShapeDtypeStruct((DEVICES, LANES), jnp.int32)
    first, rest = first_pieces(me, decoding_table)
    other_table = other_core(decoding_table)
    sent = pl.pallas_call(local_compaction, out_shape=square, in_specs=[vmem(), vmem()], out_specs=vmem(), compiler_params=SMALL, name="local_compaction")(
        lookup_keys_per_record.reshape(BLOCKS, LANES), filter_passed_flags.reshape(BLOCKS, LANES)
    )
    got = exchange(sent)
    every, ring = ring_pieces(first)
    other_every = other_core(every)
    sent = pl.pallas_call(
        regroup,
        out_shape=square,
        in_specs=[smem(), vmem()],
        out_specs=vmem(),
        compiler_params=SMALL,
        name="regroup",
    )(me, got)
    got = exchange(sent)
    held = pl.pallas_call(
        hold,
        out_shape=pltpu.VMEM((HELD, LANES), jnp.bfloat16),
        in_specs=[smem()],
        out_specs=vmem(),
        compiler_params=SMALL,
        name="hold",
    )(me)
    other_rest = [other_core(piece) for piece in rest]
    other_ring = [other_core(piece) for piece in ring[:2]]
    other_ring += [other_core(piece) for piece in ring[2:]]
    pieces = [decoding_table, every, *rest, *ring, other_table, other_every, *other_rest, *other_ring]
    pieces = [pltpu.with_memory_space_constraint(piece.reshape(-1, 2, LANES), pltpu.HBM) for piece in pieces]
    return pl.pallas_call(
        decode,
        out_shape=jax.ShapeDtypeStruct((BLOCKS * LANES, LANES), jnp.bfloat16),
        in_specs=[smem(), vmem(), vmem()] + [anywhere()] * len(pieces),
        out_specs=vmem(),
        scratch_shapes=[
            pltpu.VMEM((ENTRIES // 2 + 8, 2, LANES), jnp.bfloat16),
            pltpu.VMEM((BLOCKS, 2 * LANES, LANES), jnp.bfloat16),
            pltpu.VMEM((4, 2 * LANES, LANES), jnp.float32),
            pltpu.VMEM((BLOCKS, LANES), jnp.int32),
            pltpu.SMEM((BLOCKS, LANES), jnp.int32),
            pltpu.SemaphoreType.DMA(()),
            pltpu.SemaphoreType.DMA(()),
        ],
        compiler_params=pltpu.CompilerParams(vmem_limit_bytes=32 << 20),
        name="decode",
    )(me, got, pltpu.with_memory_space_constraint(held, pltpu.VMEM), *pieces)


def solution(mesh):
    placed = (P(ALL), P(ALL), P("dict", None))
    return jax.shard_map(steps, mesh=mesh, in_specs=placed, out_specs=P(ALL, None), check_vma=False)
```

```python
import jax
import jax.numpy as jnp
from jax import lax
from jax.experimental import pallas as pl
from jax.experimental.pallas import tpu as pltpu
from jax.sharding import PartitionSpec as P


ALL = ("rows", "dict")
LANES = 128
PRESENT = 1 << 23
DEVICES = 128
BLOCKS = 32
SHARD = 8192
RING = (2, -1, 1)
LARGE, SMALLER = (1248, 608, 608), (800, 416, 416)
BOTH = tuple(large + smaller for large, smaller in zip(LARGE, SMALLER))
REST = SHARD - 4 * BOTH[1]
ENTRIES = 8 * SHARD
HELD = 8192
SMALL = pltpu.CompilerParams(vmem_limit_bytes=8 << 20)


def iota(shape, dim):
    return lax.broadcasted_iota(jnp.int32, shape, dim)


def exact_dot(a, b):
    return jnp.dot(a.astype(jnp.bfloat16), b.astype(jnp.bfloat16), preferred_element_type=jnp.float32)


def local_compaction(keys_ref, flags_ref, out_ref):
    flags = flags_ref[...]
    rows = flags.shape[0]
    upper = jnp.where(iota((LANES, LANES), 0) <= iota((LANES, LANES), 1), 1.0, 0.0)
    below = jnp.where(iota((rows, rows), 1) < iota((rows, rows), 0), 1.0, 0.0)
    kept = flags.astype(jnp.float32)
    inclusive = exact_dot(kept, upper)
    row_sums = exact_dot(kept, jnp.ones((LANES, LANES), jnp.float32))
    position = (inclusive + exact_dot(below, row_sums)).astype(jnp.int32) - 1
    count = jnp.sum(row_sums, axis=0, keepdims=True).astype(jnp.int32)
    here = iota((rows, LANES), 0) * LANES + iota((rows, LANES), 1)
    lane = iota((rows, LANES), 1)
    item = jnp.where(flags > 0, ((here - position) << 16) | keys_ref[...], 0)
    for level in range((rows * LANES - 1).bit_length()):
        step = 1 << level
        moving = (item >> (16 + level)) & 1 == 1
        sent = jnp.where(moving, item, 0)
        if step < LANES:
            near = pltpu.roll(sent, LANES - step, 1)
            arrived = jnp.where(lane < LANES - step, near, pltpu.roll(near, rows - 1, 0))
        else:
            arrived = pltpu.roll(sent, rows - step // LANES, 0)
        item = jnp.where(moving, 0, item) | arrived
    codes = item & 0xFFFF
    counts = jnp.broadcast_to(count, (LANES - rows, LANES))
    out_ref[...] = jnp.concatenate([codes, counts], axis=0).T


def regroup(me_ref, got_ref, out_ref):
    me = me_ref[0]
    got = got_ref[...]
    shape = got.shape
    lane = iota(shape, 1)
    count = jnp.max(jnp.where(lane >= BLOCKS, got, 0), axis=1, keepdims=True)
    count = jnp.broadcast_to(count, shape)
    below = jnp.where(iota(shape, 1) < iota(shape, 0), 1.0, 0.0)
    offset = 64 * exact_dot(below, (count >> 6).astype(jnp.float32)) + exact_dot(below, (count & 63).astype(jnp.float32))
    start = offset.astype(jnp.int32) + me
    valid = (lane < BLOCKS) & (lane * LANES + me < count)
    item = jnp.where(valid, PRESENT | ((start & 127) << 16) | got, 0)
    turn = (start >> 7) & (BLOCKS - 1)
    for level in range(5):
        item = jnp.where((turn >> level) & 1 == 1, pltpu.roll(item, 1 << level, 1), item)
    odd = iota(shape, 0) & 1 == 1
    low = jnp.where(lane < BLOCKS, item, 0)
    high = jnp.where(lane < BLOCKS, pltpu.roll(item, LANES - BLOCKS, 1), 0)
    low = jnp.where(odd, pltpu.roll(low, BLOCKS, 1), low)
    high = jnp.where(odd, pltpu.roll(high, BLOCKS, 1), high)
    both = jnp.concatenate([low, high], axis=0)
    device = (start >> 12).T
    here = iota(shape, 0)
    chosen = [jnp.where(device + next_one == here, 1.0, 0.0) for next_one in (0, 1)]
    chosen = jnp.concatenate(chosen, axis=1)
    total = exact_dot(chosen, (both & 255).astype(jnp.float32))
    total += 256 * exact_dot(chosen, ((both >> 8) & 255).astype(jnp.float32))
    total += 65536 * exact_dot(chosen, (both >> 16).astype(jnp.float32))
    out_ref[...] = total.astype(jnp.int32)


def colours(x, y):
    return (x + 2 * y) & 3, (2 * x + y) & 3


def table_parts(me, half):
    x, y, z, core = (me >> 3) & 3, me >> 5, (me >> 1) & 3, (me & 1) ^ half
    a, b = colours(x, y)
    bases = [(((z + step) & 3) * 2 + core) * SHARD for step in RING]
    a_rows = list(zip(LARGE, bases))
    b_rows = list(zip(SMALLER, [base + 4 * rows for rows, base in a_rows]))

    def whole(parts, colour):
        return [(rows, base + rows * (colour & 3)) for rows, base in parts]

    def part(parts, colour, at):
        return [(rows // 2, base + rows * (colour & 3) + at * (rows // 2)) for rows, base in parts]

    places = [[(SHARD, (z * 2 + core) * SHARD)]]
    places += [[place for pair in zip(whole(a_rows, a), whole(b_rows, b)) for place in pair]]
    places += [[(REST, base + SHARD - REST)] for base in bases[1:]]
    places += [whole(a_rows, a - 1) + part(b_rows, b + 2, 0), whole(a_rows, a + 1) + part(b_rows, b + 2, 1)]
    places += [whole(b_rows, b - 1) + part(a_rows, a + 2, 0), whole(b_rows, b + 1) + part(a_rows, a + 2, 1)]
    return places


def decode(me_ref, got_ref, held_ref, *refs):
    pieces, out_ref, scratch = refs[:-11], refs[-11], refs[-10:]
    table_ref, pairs_ref, wide_ref, odd_ref, rows_ref, place_ref, scalar_ref, sem, place_sem, out_sem = scratch
    me = me_ref[0]
    for piece, places in zip(pieces, table_parts(me, 0) + table_parts(me, 1)):
        at = 0
        for rows, base in places:
            pltpu.make_async_copy(
                piece.at[pl.ds(at // 2, rows // 2)], table_ref.at[pl.ds(base >> 1, rows // 2)], sem
            ).start()
            at += rows
    table_ref[pl.ds(ENTRIES // 2, 8)] = jnp.zeros((8, 2, LANES), table_ref.dtype)

    item = got_ref[...].T[: 2 * BLOCKS]
    lane = iota(item.shape, 1)
    turn = (((item >> 16) & 127) - lane) & 127
    item = jnp.where(item > 0, (item & (PRESENT | 0xFFFF)) | (turn << 16), 0)
    for level in range(7):
        moving = (item >> (16 + level)) & 1 == 1
        item = jnp.where(moving, 0, item) | pltpu.roll(jnp.where(moving, item, 0), 1 << level, 1)
    item = item[:BLOCKS] | item[BLOCKS:]
    place_ref[...] = jnp.where(item > 0, (item & 0xFFFF) >> 1, ENTRIES // 2)
    to_scalars = pltpu.make_async_copy(place_ref, scalar_ref, place_sem)
    to_scalars.start()
    odd = jnp.concatenate([item & 1, jnp.zeros((LANES - BLOCKS, LANES), jnp.int32)], axis=0).T
    for b in range(BLOCKS):
        odd_ref[b] = jnp.broadcast_to(odd[:, b : b + 1], (LANES, LANES))
    pairs_ref[0] = jnp.zeros(pairs_ref.shape[1:], pairs_ref.dtype)
    to_scalars.wait()
    filled = table_ref.at[pl.ds(0, ENTRIES // 2)]
    pltpu.make_async_copy(filled, filled, sem).wait()

    def finish(b):
        wide_ref[...] = pairs_ref[b].astype(jnp.float32)
        second, first = wide_ref[pl.ds(1, LANES, stride=2), :], wide_ref[pl.ds(0, LANES, stride=2), :]
        row = jnp.where(odd_ref[b] == 1, second, first)
        rows_ref[b] = row.astype(rows_ref.dtype)

    def send(b):
        here = out_ref.at[pl.ds(pl.multiple_of(b * LANES, LANES), LANES)]
        pltpu.make_async_copy(rows_ref.at[b], here, out_sem).start()

    def fetch(b, _):
        before = jnp.maximum(b - 1, 0)
        finish(before)
        for j in range(LANES):
            pairs_ref[b, 2 * j : 2 * j + 2, :] = table_ref[scalar_ref[b, j]]
        pl.when(b > 0)(lambda: send(before))
        return 0

    lax.fori_loop(0, BLOCKS, fetch, 0)
    finish(BLOCKS - 1)
    send(BLOCKS - 1)
    pltpu.make_async_copy(out_ref, out_ref, out_sem).wait()


def moved(x, by):
    pairs = []
    for me in range(DEVICES):
        place = ((me >> 3) & 3, me >> 5, (me >> 1) & 3, me & 1)
        to_x, to_y, to_z, to_core = by(*place)
        pairs.append((me, ((to_y & 3) * 4 + (to_x & 3)) * 8 + (to_z & 3) * 2 + to_core))
    return lax.ppermute(x, ALL, pairs)


def along_z(pieces, steps):
    return [
        moved(piece, lambda x, y, z, core, step=step: (x, y, z - step, core)) for piece, step in zip(pieces, steps)
    ]


def other_core(piece):
    return moved(piece, lambda x, y, z, core: (x, y, z, 1 - core))


def cut(me_ref, table_ref, far_ref, near_ref, sems):
    a, b = colours((me_ref[0] >> 3) & 3, me_ref[0] >> 5)
    copies = []
    for out, large, smaller in ((far_ref, LARGE[0], SMALLER[0]), (near_ref, LARGE[1], SMALLER[1])):
        for at, to, rows in ((large * a, 0, large), (4 * large + smaller * b, large, smaller)):
            copies.append(
                pltpu.make_async_copy(table_ref.at[pl.ds(at, rows)], out.at[pl.ds(to, rows)], sems.at[len(copies)])
            )
    for copy in copies:
        copy.start()
    for copy in copies:
        copy.wait()


def join(*refs):
    pieces, joined, all_ref = refs[: len(RING)], refs[len(RING) : -1], refs[-1]
    for number, out in enumerate(joined):
        to = 0
        for share in (1, 2):
            for large, smaller, piece in zip(LARGE, SMALLER, pieces):
                begin, rows = (0, large) if (number < 2) == (share == 1) else (large, smaller)
                rows //= share
                begin += rows * (number % 2) * (share - 1)
                out[to : to + rows, :] = piece[begin : begin + rows, :]
                to += rows
    to = 0
    for rows, piece in zip(BOTH, pieces):
        all_ref[to : to + rows, :] = piece[...]
        to += rows


def first_pieces(me, table):
    far, near = pl.pallas_call(
        cut,
        out_shape=[pltpu.VMEM((rows, LANES), table.dtype) for rows in BOTH[:2]],
        in_specs=[smem(), anywhere()],
        out_specs=[vmem()] * 2,
        scratch_shapes=[pltpu.SemaphoreType.DMA((4,))],
        name="cut",
    )(me, pltpu.with_memory_space_constraint(table, pltpu.HBM))
    first = along_z([far, near, near], RING)
    rest = along_z([table[SHARD - REST :]] * 2, RING[1:])
    return first, rest


def ring_pieces(first):
    rows = [sum(LARGE) + sum(SMALLER) // 2] * 2 + [sum(SMALLER) + sum(LARGE) // 2] * 2
    *sent, every = pl.pallas_call(
        join,
        out_shape=[pltpu.VMEM((count, LANES), first[0].dtype) for count in rows]
        + [jax.ShapeDtypeStruct((sum(BOTH), LANES), first[0].dtype)],
        in_specs=[vmem()] * len(first),
        out_specs=[vmem()] * 5,
        compiler_params=SMALL,
        name="join",
    )(*first)
    ring = [
        moved(sent[0], lambda x, y, z, core: (x + 1, y, z, core)),
        moved(sent[1], lambda x, y, z, core: (x - 1, y, z, core)),
    ]
    ring += [
        moved(sent[2], lambda x, y, z, core: (x, y + 1, z, core)),
        moved(sent[3], lambda x, y, z, core: (x, y - 1, z, core)),
    ]
    return every, ring


def anywhere():
    return pl.BlockSpec(memory_space=pl.ANY)


def hold(me_ref, held_ref):
    held_ref[:16, :] = jnp.zeros((16, LANES), held_ref.dtype)


def vmem():
    return pl.BlockSpec(memory_space=pltpu.VMEM)


def smem():
    return pl.BlockSpec(memory_space=pltpu.SMEM)


def exchange(x):
    return lax.all_to_all(x, ALL, 0, 0, tiled=True)


def steps(lookup_keys_per_record, filter_passed_flags, decoding_table):
    me = lax.axis_index(ALL).astype(jnp.int32).reshape(1)
    square = jax.ShapeDtypeStruct((DEVICES, LANES), jnp.int32)
    first, rest = first_pieces(me, decoding_table)
    other_table = other_core(decoding_table)
    sent = pl.pallas_call(local_compaction, out_shape=square, in_specs=[vmem(), vmem()], out_specs=vmem(), compiler_params=SMALL, name="local_compaction")(
        lookup_keys_per_record.reshape(BLOCKS, LANES), filter_passed_flags.reshape(BLOCKS, LANES)
    )
    got = exchange(sent)
    every, ring = ring_pieces(first)
    other_every = other_core(every)
    sent = pl.pallas_call(
        regroup,
        out_shape=square,
        in_specs=[smem(), vmem()],
        out_specs=vmem(),
        compiler_params=SMALL,
        name="regroup",
    )(me, got)
    got = exchange(sent)
    held = pl.pallas_call(
        hold,
        out_shape=pltpu.VMEM((HELD, LANES), jnp.bfloat16),
        in_specs=[smem()],
        out_specs=vmem(),
        compiler_params=SMALL,
        name="hold",
    )(me)
    other_rest = []
    for piece in rest:
        other_rest.append(other_core(piece))
    other_ring = [other_core(piece) for piece in ring[:2]]
    other_ring += [other_core(piece) for piece in ring[2:]]
    pieces = [decoding_table, every, *rest, *ring, other_table, other_every, *other_rest, *other_ring]
    pieces = [pltpu.with_memory_space_constraint(piece.reshape(-1, 2, LANES), pltpu.HBM) for piece in pieces]
    return pl.pallas_call(
        decode,
        out_shape=jax.ShapeDtypeStruct((BLOCKS * LANES, LANES), jnp.bfloat16),
        in_specs=[smem(), vmem(), vmem()] + [anywhere()] * len(pieces),
        out_specs=anywhere(),
        scratch_shapes=[
            pltpu.VMEM((ENTRIES // 2 + 8, 2, LANES), jnp.bfloat16),
            pltpu.VMEM((BLOCKS, 2 * LANES, LANES), jnp.bfloat16),
            pltpu.VMEM((2 * LANES, LANES), jnp.float32),
            pltpu.VMEM((BLOCKS, LANES, LANES), jnp.int32),
            pltpu.VMEM((BLOCKS, LANES, LANES), jnp.bfloat16),
            pltpu.VMEM((BLOCKS, LANES), jnp.int32),
            pltpu.SMEM((BLOCKS, LANES), jnp.int32),
            pltpu.SemaphoreType.DMA(()),
            pltpu.SemaphoreType.DMA(()),
            pltpu.SemaphoreType.DMA(()),
        ],
        compiler_params=pltpu.CompilerParams(vmem_limit_bytes=32 << 20),
        name="decode",
    )(me, got, pltpu.with_memory_space_constraint(held, pltpu.VMEM), *pieces)


def solution(mesh):
    placed = (P(ALL), P(ALL), P("dict", None))
    return jax.shard_map(steps, mesh=mesh, in_specs=placed, out_specs=P(ALL, None), check_vma=False)
```

```python
import jax
import jax.numpy as jnp
from jax import lax
from jax.experimental import pallas as pl
from jax.experimental.pallas import tpu as pltpu
from jax.sharding import PartitionSpec as P


ALL = ("rows", "dict")
LANES = 128
PRESENT = 1 << 23
DEVICES = 128
BLOCKS = 32
SHARD = 8192
RING = (2, -1, 1)
LARGE, SMALLER = (1216, 640, 640), (832, 448, 448)
BOTH = tuple(large + smaller for large, smaller in zip(LARGE, SMALLER))
REST = SHARD - 4 * BOTH[1]
ENTRIES = 8 * SHARD
HELD = 8192
SMALL = pltpu.CompilerParams(vmem_limit_bytes=8 << 20)


def iota(shape, dim):
    return lax.broadcasted_iota(jnp.int32, shape, dim)


def exact_dot(a, b):
    return jnp.dot(a.astype(jnp.bfloat16), b.astype(jnp.bfloat16), preferred_element_type=jnp.float32)


def local_compaction(keys_ref, flags_ref, out_ref):
    flags = flags_ref[...]
    rows = flags.shape[0]
    upper = jnp.where(iota((LANES, LANES), 0) <= iota((LANES, LANES), 1), 1.0, 0.0)
    below = jnp.where(iota((rows, rows), 1) < iota((rows, rows), 0), 1.0, 0.0)
    kept = flags.astype(jnp.float32)
    inclusive = exact_dot(kept, upper)
    row_sums = exact_dot(kept, jnp.ones((LANES, LANES), jnp.float32))
    position = (inclusive + exact_dot(below, row_sums)).astype(jnp.int32) - 1
    count = jnp.sum(row_sums, axis=0, keepdims=True).astype(jnp.int32)
    here = iota((rows, LANES), 0) * LANES + iota((rows, LANES), 1)
    lane = iota((rows, LANES), 1)
    item = jnp.where(flags > 0, ((here - position) << 16) | keys_ref[...], 0)
    for level in range((rows * LANES - 1).bit_length()):
        step = 1 << level
        moving = (item >> (16 + level)) & 1 == 1
        sent = jnp.where(moving, item, 0)
        if step < LANES:
            near = pltpu.roll(sent, LANES - step, 1)
            arrived = jnp.where(lane < LANES - step, near, pltpu.roll(near, rows - 1, 0))
        else:
            arrived = pltpu.roll(sent, rows - step // LANES, 0)
        item = jnp.where(moving, 0, item) | arrived
    codes = item & 0xFFFF
    counts = jnp.broadcast_to(count, (LANES - rows, LANES))
    out_ref[...] = jnp.concatenate([codes, counts], axis=0).T


def regroup(me_ref, got_ref, out_ref):
    me = me_ref[0]
    got = got_ref[...]
    shape = got.shape
    lane = iota(shape, 1)
    count = jnp.max(jnp.where(lane >= BLOCKS, got, 0), axis=1, keepdims=True)
    count = jnp.broadcast_to(count, shape)
    below = jnp.where(iota(shape, 1) < iota(shape, 0), 1.0, 0.0)
    offset = 64 * exact_dot(below, (count >> 6).astype(jnp.float32)) + exact_dot(below, (count & 63).astype(jnp.float32))
    start = offset.astype(jnp.int32) + me
    valid = (lane < BLOCKS) & (lane * LANES + me < count)
    item = jnp.where(valid, PRESENT | ((start & 127) << 16) | got, 0)
    turn = (start >> 7) & (BLOCKS - 1)
    for level in range(5):
        item = jnp.where((turn >> level) & 1 == 1, pltpu.roll(item, 1 << level, 1), item)
    odd = iota(shape, 0) & 1 == 1
    low = jnp.where(lane < BLOCKS, item, 0)
    high = jnp.where(lane < BLOCKS, pltpu.roll(item, LANES - BLOCKS, 1), 0)
    low = jnp.where(odd, pltpu.roll(low, BLOCKS, 1), low)
    high = jnp.where(odd, pltpu.roll(high, BLOCKS, 1), high)
    both = jnp.concatenate([low, high], axis=0)
    device = (start >> 12).T
    here = iota(shape, 0)
    chosen = [jnp.where(device + next_one == here, 1.0, 0.0) for next_one in (0, 1)]
    chosen = jnp.concatenate(chosen, axis=1)
    total = exact_dot(chosen, (both & 255).astype(jnp.float32))
    total += 256 * exact_dot(chosen, ((both >> 8) & 255).astype(jnp.float32))
    total += 65536 * exact_dot(chosen, (both >> 16).astype(jnp.float32))
    out_ref[...] = total.astype(jnp.int32)


def colours(x, y):
    return (x + 2 * y) & 3, (2 * x + y) & 3


def table_parts(me, half):
    x, y, z, core = (me >> 3) & 3, me >> 5, (me >> 1) & 3, (me & 1) ^ half
    a, b = colours(x, y)
    bases = [(((z + step) & 3) * 2 + core) * SHARD for step in RING]
    a_rows = list(zip(LARGE, bases))
    b_rows = list(zip(SMALLER, [base + 4 * rows for rows, base in a_rows]))

    def whole(parts, colour):
        return [(rows, base + rows * (colour & 3)) for rows, base in parts]

    def part(parts, colour, at):
        return [(rows // 2, base + rows * (colour & 3) + at * (rows // 2)) for rows, base in parts]

    places = [[(SHARD, (z * 2 + core) * SHARD)]]
    places += [[place for pair in zip(whole(a_rows, a), whole(b_rows, b)) for place in pair]]
    places += [[(REST, base + SHARD - REST)] for base in bases[1:]]
    places += [whole(a_rows, a - 1) + part(b_rows, b + 2, 0), whole(a_rows, a + 1) + part(b_rows, b + 2, 1)]
    places += [whole(b_rows, b - 1) + part(a_rows, a + 2, 0), whole(b_rows, b + 1) + part(a_rows, a + 2, 1)]
    return places


def decode(me_ref, got_ref, held_ref, *refs):
    pieces, out_ref, scratch = refs[:-11], refs[-11], refs[-10:]
    table_ref, pairs_ref, wide_ref, odd_ref, rows_ref, place_ref, scalar_ref, sem, place_sem, out_sem = scratch
    me = me_ref[0]
    work = sorted(zip(pieces, table_parts(me, 0) + table_parts(me, 1)), key=lambda item: -item[0].shape[0] // len(item[1]))
    for piece, places in work:
        at = 0
        for rows, base in places:
            pltpu.make_async_copy(
                piece.at[pl.ds(at // 2, rows // 2)], table_ref.at[pl.ds(base >> 1, rows // 2)], sem
            ).start()
            at += rows
    table_ref[pl.ds(ENTRIES // 2, 8)] = jnp.zeros((8, 2, LANES), table_ref.dtype)

    item = got_ref[...].T[: 2 * BLOCKS]
    lane = iota(item.shape, 1)
    turn = (((item >> 16) & 127) - lane) & 127
    item = jnp.where(item > 0, (item & (PRESENT | 0xFFFF)) | (turn << 16), 0)
    for level in range(7):
        moving = (item >> (16 + level)) & 1 == 1
        item = jnp.where(moving, 0, item) | pltpu.roll(jnp.where(moving, item, 0), 1 << level, 1)
    item = item[:BLOCKS] | item[BLOCKS:]
    place_ref[...] = jnp.where(item > 0, (item & 0xFFFF) >> 1, ENTRIES // 2)
    to_scalars = pltpu.make_async_copy(place_ref, scalar_ref, place_sem)
    to_scalars.start()
    odd = jnp.concatenate([item & 1, jnp.zeros((LANES - BLOCKS, LANES), jnp.int32)], axis=0).T
    for b in range(BLOCKS):
        odd_ref[b] = jnp.broadcast_to(odd[:, b : b + 1], (LANES, LANES))
    pairs_ref[0] = jnp.zeros(pairs_ref.shape[1:], pairs_ref.dtype)
    to_scalars.wait()
    filled = table_ref.at[pl.ds(0, ENTRIES // 2)]
    pltpu.make_async_copy(filled, filled, sem).wait()

    def finish(b):
        wide_ref[...] = pairs_ref[b].astype(jnp.float32)
        second, first = wide_ref[pl.ds(1, LANES, stride=2), :], wide_ref[pl.ds(0, LANES, stride=2), :]
        row = jnp.where(odd_ref[b] == 1, second, first)
        rows_ref[b] = row.astype(rows_ref.dtype)

    def send(b):
        here = out_ref.at[pl.ds(pl.multiple_of(b * LANES, LANES), LANES)]
        pltpu.make_async_copy(rows_ref.at[b], here, out_sem).start()

    def fetch(b, _):
        before = jnp.maximum(b - 1, 0)
        finish(before)
        for j in range(LANES):
            pairs_ref[b, 2 * j : 2 * j + 2, :] = table_ref[scalar_ref[b, j]]
        pl.when(b > 0)(lambda: send(before))
        return 0

    lax.fori_loop(0, BLOCKS, fetch, 0)
    finish(BLOCKS - 1)
    send(BLOCKS - 1)
    pltpu.make_async_copy(out_ref, out_ref, out_sem).wait()


def moved(x, by):
    pairs = []
    for me in range(DEVICES):
        place = ((me >> 3) & 3, me >> 5, (me >> 1) & 3, me & 1)
        to_x, to_y, to_z, to_core = by(*place)
        pairs.append((me, ((to_y & 3) * 4 + (to_x & 3)) * 8 + (to_z & 3) * 2 + to_core))
    return lax.ppermute(x, ALL, pairs)


def along_z(pieces, steps):
    return [
        moved(piece, lambda x, y, z, core, step=step: (x, y, z - step, core)) for piece, step in zip(pieces, steps)
    ]


def other_core(piece):
    return moved(piece, lambda x, y, z, core: (x, y, z, 1 - core))


def cut(me_ref, table_ref, far_ref, near_ref, sems):
    a, b = colours((me_ref[0] >> 3) & 3, me_ref[0] >> 5)
    copies = []
    for out, large, smaller in ((far_ref, LARGE[0], SMALLER[0]), (near_ref, LARGE[1], SMALLER[1])):
        for at, to, rows in ((large * a, 0, large), (4 * large + smaller * b, large, smaller)):
            copies.append(
                pltpu.make_async_copy(table_ref.at[pl.ds(at, rows)], out.at[pl.ds(to, rows)], sems.at[len(copies)])
            )
    for copy in copies:
        copy.start()
    for copy in copies:
        copy.wait()


def join(*refs):
    pieces, joined, all_ref = refs[: len(RING)], refs[len(RING) : -1], refs[-1]
    for number, out in enumerate(joined):
        to = 0
        for share in (1, 2):
            for large, smaller, piece in zip(LARGE, SMALLER, pieces):
                begin, rows = (0, large) if (number < 2) == (share == 1) else (large, smaller)
                rows //= share
                begin += rows * (number % 2) * (share - 1)
                out[to : to + rows, :] = piece[begin : begin + rows, :]
                to += rows
    to = 0
    for rows, piece in zip(BOTH, pieces):
        all_ref[to : to + rows, :] = piece[...]
        to += rows


def first_pieces(me, table):
    far, near = pl.pallas_call(
        cut,
        out_shape=[pltpu.VMEM((rows, LANES), table.dtype) for rows in BOTH[:2]],
        in_specs=[smem(), anywhere()],
        out_specs=[vmem()] * 2,
        scratch_shapes=[pltpu.SemaphoreType.DMA((4,))],
        name="cut",
    )(me, pltpu.with_memory_space_constraint(table, pltpu.HBM))
    first = along_z([far, near, near], RING)
    rest = along_z([table[SHARD - REST :]] * 2, RING[1:])
    return first, rest


def ring_pieces(first):
    rows = [sum(LARGE) + sum(SMALLER) // 2] * 2 + [sum(SMALLER) + sum(LARGE) // 2] * 2
    *sent, every = pl.pallas_call(
        join,
        out_shape=[pltpu.VMEM((count, LANES), first[0].dtype) for count in rows]
        + [jax.ShapeDtypeStruct((sum(BOTH), LANES), first[0].dtype)],
        in_specs=[vmem()] * len(first),
        out_specs=[vmem()] * 5,
        compiler_params=SMALL,
        name="join",
    )(*first)
    ring = [
        moved(sent[0], lambda x, y, z, core: (x + 1, y, z, core)),
        moved(sent[1], lambda x, y, z, core: (x - 1, y, z, core)),
    ]
    ring += [
        moved(sent[2], lambda x, y, z, core: (x, y + 1, z, core)),
        moved(sent[3], lambda x, y, z, core: (x, y - 1, z, core)),
    ]
    return every, ring


def anywhere():
    return pl.BlockSpec(memory_space=pl.ANY)


def hold(me_ref, held_ref):
    held_ref[:16, :] = jnp.zeros((16, LANES), held_ref.dtype)


def vmem():
    return pl.BlockSpec(memory_space=pltpu.VMEM)


def smem():
    return pl.BlockSpec(memory_space=pltpu.SMEM)


def exchange(x):
    return lax.all_to_all(x, ALL, 0, 0, tiled=True)


def steps(lookup_keys_per_record, filter_passed_flags, decoding_table):
    me = lax.axis_index(ALL).astype(jnp.int32).reshape(1)
    square = jax.ShapeDtypeStruct((DEVICES, LANES), jnp.int32)
    first, rest = first_pieces(me, decoding_table)
    other_table = other_core(decoding_table)
    sent = pl.pallas_call(local_compaction, out_shape=square, in_specs=[vmem(), vmem()], out_specs=vmem(), compiler_params=SMALL, name="local_compaction")(
        lookup_keys_per_record.reshape(BLOCKS, LANES), filter_passed_flags.reshape(BLOCKS, LANES)
    )
    got = exchange(sent)
    every, ring = ring_pieces(first)
    other_every = other_core(every)
    sent = pl.pallas_call(
        regroup,
        out_shape=square,
        in_specs=[smem(), vmem()],
        out_specs=vmem(),
        compiler_params=SMALL,
        name="regroup",
    )(me, got)
    got = exchange(sent)
    held = pl.pallas_call(
        hold,
        out_shape=pltpu.VMEM((HELD, LANES), jnp.bfloat16),
        in_specs=[smem()],
        out_specs=vmem(),
        compiler_params=SMALL,
        name="hold",
    )(me)
    other_rest = [other_core(piece) for piece in rest]
    other_ring = [other_core(piece) for piece in ring[:2]]
    other_ring += [other_core(piece) for piece in ring[2:]]
    pieces = [decoding_table, every, *rest, *ring, other_table, other_every, *other_rest, *other_ring]
    pieces = [pltpu.with_memory_space_constraint(piece.reshape(-1, 2, LANES), pltpu.HBM) for piece in pieces]
    return pl.pallas_call(
        decode,
        out_shape=jax.ShapeDtypeStruct((BLOCKS * LANES, LANES), jnp.bfloat16),
        in_specs=[smem(), vmem(), vmem()] + [anywhere()] * len(pieces),
        out_specs=anywhere(),
        scratch_shapes=[
            pltpu.VMEM((ENTRIES // 2 + 8, 2, LANES), jnp.bfloat16),
            pltpu.VMEM((BLOCKS, 2 * LANES, LANES), jnp.bfloat16),
            pltpu.VMEM((2 * LANES, LANES), jnp.float32),
            pltpu.VMEM((BLOCKS, LANES, LANES), jnp.int32),
            pltpu.VMEM((BLOCKS, LANES, LANES), jnp.bfloat16),
            pltpu.VMEM((BLOCKS, LANES), jnp.int32),
            pltpu.SMEM((BLOCKS, LANES), jnp.int32),
            pltpu.SemaphoreType.DMA(()),
            pltpu.SemaphoreType.DMA(()),
            pltpu.SemaphoreType.DMA(()),
        ],
        compiler_params=pltpu.CompilerParams(vmem_limit_bytes=32 << 20),
        name="decode",
    )(me, got, pltpu.with_memory_space_constraint(held, pltpu.VMEM), *pieces)


def solution(mesh):
    placed = (P(ALL), P(ALL), P("dict", None))
    return jax.shard_map(steps, mesh=mesh, in_specs=placed, out_specs=P(ALL, None), check_vma=False)
```
